256 devices in a mesh: var: 8 (over z), lat: 4 (over x), lon: 8 (over y, core).
Axes of the slice: x: 4, y: 4, z: 8, core: 2. Of those that a mesh axis runs over, the one named last changes fastest.
Arguments:
- state: bfloat16 [1, 256, 384, 1024], P(None, 'var', 'lat', 'lon'), may hold values from -6 to 6
- weights_in: bfloat16 [2, 256, 256], replicated, may hold values from -0.25 to 0.25
- bias_in: float32 [2, 256], replicated, may hold values from -3 to 3
- weights_out: bfloat16 [2, 256, 256], replicated, may hold values from -2 to 2
Outputs:
- field: bfloat16 [1, 256, 384, 1024], P(None, 'var', 'lat', 'lon')
- zonal: float32 [1, 256, 384], P(None, 'var', 'lat')
- energy: float32 [256], P('var')
The draws below stay inside these ranges and needn't reach their ends.
All inputs are finite; a program needn't handle non-finite values.
Results may differ from the reference program's by a relative error of at most 0.012.
Values may be sent and summed in bfloat16 or wider, within the bound.
A program may use at most 64 MiB of HBM per device.

```python
import math
import jax
import jax.numpy as jnp
from jax import lax

BATCH = 1
C = 256
HID = 256
LAT = 384
LON = 1024
MLAT = 96
MLON = 96


def levels(own_key, shape, split, smallest, high):
    gain = 1.0
    for dim, blocks in split:
        steps = jax.random.uniform(jax.random.fold_in(jax.random.fold_in(own_key, 6), dim), (blocks,), jnp.float32, smallest / len(split), high / len(split))
        gain = gain * jnp.repeat(jnp.exp(steps), shape[dim] // blocks).reshape((-1,) + (1,) * (len(shape) - 1 - dim))
    return gain


def gaussian(own_key, extent, deviation, reach, split=(), held_as=jnp.bfloat16):
    entries = deviation * jax.random.normal(own_key, extent, jnp.float32)
    if split:
        entries = entries * levels(own_key, extent, split, -0.22, 0.18)
    return jnp.clip(entries, -reach, reach).astype(held_as)


def setup_inputs(seed: int = 0) -> dict:
    arg_keys = jax.random.split(jax.random.key(seed), 5)
    state = gaussian(arg_keys[0], (BATCH, C, LAT, LON), 1.0, 6.0, ((1, 8), (2, 4), (3, 8)))
    weights_in = gaussian(arg_keys[1], (2, HID, C), (2 * C) ** -0.5, 0.25)
    bias_in = gaussian(arg_keys[2], (2, HID), 0.5, 3.0, (), jnp.float32)
    weights_out = gaussian(arg_keys[3], (2, C, HID), (HID // 32) ** -0.5, 2.0)
    return dict(state=state, weights_in=weights_in, bias_in=bias_in, weights_out=weights_out)


def lon_forward(first, count):
    index = first + jnp.arange(count, dtype=jnp.int32)
    modes = jnp.arange(MLON, dtype=jnp.int32)
    phase = index[:, None] * modes[None, :] % LON
    angle = phase.astype(jnp.float32) * (2.0 * math.pi / LON)
    scale = 1.0 / math.sqrt(LAT * LON)
    return (jnp.stack([jnp.cos(angle), -jnp.sin(angle)], 1) * scale).astype(jnp.bfloat16)

def lat_forward(first, count):
    freqs = jnp.arange(MLAT, dtype=jnp.int32) - MLAT // 2
    index = first + jnp.arange(count, dtype=jnp.int32)
    phase = jnp.mod(freqs[:, None] * index[None, :], LAT)
    angle = phase.astype(jnp.float32) * (2.0 * math.pi / LAT)
    cosine, sine = (jnp.cos(angle), jnp.sin(angle))
    return jnp.stack([jnp.stack([cosine, sine]), jnp.stack([-sine, cosine])])

def lat_inverse(first, count):
    freqs = jnp.arange(MLAT, dtype=jnp.int32) - MLAT // 2
    index = first + jnp.arange(count, dtype=jnp.int32)
    phase = jnp.mod(index[:, None] * freqs[None, :], LAT)
    angle = phase.astype(jnp.float32) * (2.0 * math.pi / LAT)
    cosine, sine = (jnp.cos(angle), jnp.sin(angle))
    return jnp.stack([jnp.stack([cosine, -sine]), jnp.stack([sine, cosine])]).astype(jnp.bfloat16)

def lon_inverse(first, count):
    modes = jnp.arange(MLON, dtype=jnp.int32)
    index = first + jnp.arange(count, dtype=jnp.int32)
    phase = modes[:, None] * index[None, :] % LON
    angle = phase.astype(jnp.float32) * (2.0 * math.pi / LON)
    factor = jnp.where(modes == 0, 1.0, 2.0).astype(jnp.float32)[:, None] / math.sqrt(LAT * LON)
    return jnp.stack([factor * jnp.cos(angle), -factor * jnp.sin(angle)]).astype(jnp.bfloat16)

def area_weights(first, count):
    index = first + jnp.arange(count, dtype=jnp.int32)
    return jnp.cos(math.pi * ((index.astype(jnp.float32) + 0.5) / LAT - 0.5))

def complex_block(pair):
    real_part, imag_part = (pair[0], pair[1])
    return jnp.stack([jnp.stack([real_part, -imag_part], 1), jnp.stack([imag_part, real_part], 1)], 0)

def reference(state, weights_in, bias_in, weights_out):
    ltab = lon_forward(0, LON).astype(jnp.float32)
    qtab = lat_forward(0, LAT)
    rtab = lat_inverse(0, LAT).astype(jnp.float32)
    htab = lon_inverse(0, LON).astype(jnp.float32)
    block_in = complex_block(weights_in).astype(jnp.float32)
    block_out = complex_block(weights_out).astype(jnp.float32)
    weights = area_weights(0, LAT)

    def single(sample):
        lonspec = jnp.einsum('cnl,lpk->pcnk', sample.astype(jnp.float32), ltab)
        spectrum = jnp.einsum('qpjn,pcnk->qcjk', qtab, lonspec, precision=lax.Precision.HIGHEST).astype(jnp.bfloat16)
        hidden = jnp.einsum('qhpc,pcjk->qhjk', block_in, spectrum.astype(jnp.float32)) + bias_in[:, :, None, None]
        hidden = jnp.maximum(hidden, 0.0).astype(jnp.bfloat16)
        mixed = jnp.einsum('qoph,phjk->qojk', block_out, hidden.astype(jnp.float32)).astype(jnp.bfloat16)
        latback = jnp.einsum('qpnj,pojk->qonk', rtab, mixed.astype(jnp.float32)).astype(jnp.bfloat16)
        result = jnp.einsum('ponk,pkl->onl', latback.astype(jnp.float32), htab)
        active = jax.nn.gelu(result, approximate=False)
        squares = lax.optimization_barrier(jnp.sum(lax.optimization_barrier(jnp.sum(active * active, -1)) * weights[None, :], -1))
        return (active.astype(jnp.bfloat16), lax.optimization_barrier(jnp.mean(active, -1)), squares)
    field, zonal, parts = lax.map(single, state)
    energy = lax.optimization_barrier(jnp.sum(parts, 0)) / (BATCH * LON * jnp.sum(weights))
    return (field, zonal, energy)
```

```python
import math

import jax
import jax.numpy as jnp
import numpy as np
from jax import lax
from jax.experimental import pallas as pl
from jax.experimental.pallas import tpu as pltpu
from jax.sharding import PartitionSpec as P

LAT = 384
LON = 1024
MLAT = 96
MLON = 96
NVAR = 8
NLAT = 4
NLON = 8
PLANE = NLAT * NLON
CD = 32
RD = LAT // NLAT
ND = LON // NLON
JO = MLAT // PLANE
MESH = pl.DeviceIdType.MESH
BF = jnp.bfloat16
F32 = jnp.float32


def tables():
    k = np.arange(MLON)
    n = np.arange(LON)
    angle = 2.0 * np.pi / LON * ((n[:, None] * k[None, :]) % LON)
    scale = 1.0 / math.sqrt(LAT * LON)
    etab = np.zeros((LON, 256), np.float32)
    etab[:, :MLON] = np.cos(angle) * scale
    etab[:, 128 : 128 + MLON] = -np.sin(angle) * scale
    weight = np.where(k == 0, 1.0, 2.0)[:, None] * scale
    full = np.zeros((256, LON), np.float32)
    full[:MLON] = weight * np.cos(angle.T)
    full[128 : 128 + MLON] = -weight * np.sin(angle.T)
    htab = full.reshape(256, NLON, ND).transpose(1, 0, 2)
    r = np.arange(LAT)
    freqs = np.arange(MLAT) - MLAT // 2
    turn = 2.0 * np.pi / LAT * np.mod(freqs[:, None] * r[None, :], LAT)
    cosine, sine = np.cos(turn), np.sin(turn)
    forward = np.zeros((PLANE, 8, 2, LAT), np.float32)
    forward[:, 0:3, 0] = cosine.reshape(PLANE, JO, LAT)
    forward[:, 0:3, 1] = sine.reshape(PLANE, JO, LAT)
    forward[:, 3:6, 0] = -sine.reshape(PLANE, JO, LAT)
    forward[:, 3:6, 1] = cosine.reshape(PLANE, JO, LAT)
    qtab = forward.reshape(PLANE * 8, 2 * LAT)
    rtab = qtab.T
    area = np.cos(np.pi * ((r + 0.5) / LAT - 0.5))
    gtab = np.broadcast_to(area.reshape(NLAT, 1, RD), (NLAT, 8, RD))
    bf = lambda t: np.ascontiguousarray(t).astype(jnp.bfloat16)
    return (
        bf(etab),
        bf(qtab),
        bf(rtab),
        bf(htab),
        np.ascontiguousarray(gtab).astype(np.float32),
        float(LON * area.sum()),
    )


def kernel(
    total_area,
    state,
    etab,
    qtab,
    rtab,
    htab,
    gtab,
    win,
    bias,
    wout,
    field,
    zonal,
    energy,
    st,
    ev,
    qv,
    rv,
    hv,
    gv,
    wiv,
    wov,
    bcol,
    xin,
    lv,
    sbuf,
    srecv,
    xf,
    xall,
    mf,
    mbuf,
    mrecv,
    lbv,
    fs,
    zst,
    strec,
    load_sem,
    s1,
    r1,
    s2,
    r2,
    s3,
    r3,
    s4,
    r4,
    s5,
    r5,
    s6,
    r6,
):
    v = lax.axis_index("var")
    a = lax.axis_index("lat")
    b = lax.axis_index("lon")
    me = a * NLON + b
    y, core = lax.div(b, 2), lax.rem(b, 2)

    def plane(d):
        part = lax.rem(d, 8)
        pa = lax.rem(a + lax.div(d, 8), NLAT)
        py = lax.rem(y + lax.div(part, 2), 4)
        pc = lax.rem(core + part, 2)
        return pa, py * 2 + pc

    loads = [
        pltpu.make_async_copy(src, dst, load_sem.at[i])
        for i, (src, dst) in enumerate(
            [
                (state.at[0], st),
                (etab, ev),
                (qtab, qv),
                (win, wiv),
                (wout, wov),
                (rtab, rv),
                (htab, hv),
                (gtab, gv),
            ]
        )
    ]
    for load in loads:
        load.start()

    barrier = pltpu.get_barrier_semaphore()

    def greet(d, _):
        pa, pb = plane(d)
        pl.semaphore_signal(barrier, inc=1, device_id={"lat": pa, "lon": pb}, device_id_type=MESH)
        return 0

    lax.fori_loop(1, PLANE, greet, 0)

    def greet_var(d, _):
        pv = lax.rem(v + d, NVAR)
        pl.semaphore_signal(barrier, inc=1, device_id={"var": pv}, device_id_type=MESH)
        return 0

    lax.fori_loop(1, NVAR, greet_var, 0)
    bcol[...] = jnp.zeros_like(bcol)
    bcol[0:2, :] = bias[...]
    turned = jnp.transpose(bcol[...])
    bias_r = jnp.broadcast_to(turned[:, 0:1], (256, 128))
    bias_i = jnp.broadcast_to(turned[:, 1:2], (256, 128))
    mf[...] = jnp.zeros_like(mf)
    zst[...] = jnp.zeros_like(zst)
    loads[0].wait()
    pl.semaphore_wait(barrier, PLANE - 1 + NVAR - 1)

    def send1(d, _):
        pa, pb = plane(d)
        pltpu.make_async_remote_copy(
            src_ref=st.at[pa * NLON + pb],
            dst_ref=xin.at[me],
            send_sem=s1.at[d],
            recv_sem=r1.at[me],
            device_id={"lat": pa, "lon": pb},
            device_id_type=MESH,
        ).start()
        return 0

    lax.fori_loop(1, PLANE, send1, 0)
    xin[me] = st[me]

    def copy1(d, slot, pa, pb):
        return pltpu.make_async_remote_copy(
            src_ref=st.at[slot],
            dst_ref=xin.at[slot],
            send_sem=s1.at[d],
            recv_sem=r1.at[slot],
            device_id={"lat": pa, "lon": pb},
            device_id_type=MESH,
        )

    loads[1].wait()
    for da in range(NLAT):

        def wait1(d, _):
            pa, pb = plane(d)
            copy1(d, pa * NLON + pb, pa, pb).wait_recv()
            return 0

        lax.fori_loop(max(1, da * 8), da * 8 + 8, wait1, 0)
        pa = lax.rem(a + da, NLAT)
        rows = jnp.concatenate([xin[pa * NLON + i] for i in range(NLON)], axis=1)
        lv[pa] = jnp.dot(rows, ev[...], preferred_element_type=F32).astype(BF)

    loads[2].wait()
    lon = lv[...].reshape(LAT, 256)
    spec = jnp.dot(qv[:, 0:LAT], lon[:, 0:128], preferred_element_type=F32)
    spec += jnp.dot(qv[:, LAT : 2 * LAT], lon[:, 128:256], preferred_element_type=F32)
    sbuf[...] = spec.reshape(PLANE, 8, 128).astype(BF)

    def copy2(d, src, dst, pa, pb):
        return pltpu.make_async_remote_copy(
            src_ref=sbuf.at[src],
            dst_ref=srecv.at[dst],
            send_sem=s2.at[d],
            recv_sem=r2.at[dst],
            device_id={"lat": pa, "lon": pb},
            device_id_type=MESH,
        )

    def send2(d, _):
        pa, pb = plane(d)
        copy2(d, pa * NLON + pb, me, pa, pb).start()
        return 0

    lax.fori_loop(1, PLANE, send2, 0)
    srecv[me] = sbuf[me]

    def wait2(d, _):
        pa, pb = plane(d)
        slot = pa * NLON + pb
        copy2(d, slot, slot, pa, pb).wait_recv()
        return 0

    lax.fori_loop(1, PLANE, wait2, 0)
    xf[...] = srecv[...].astype(F32).reshape(PLANE * 8, 128)
    t = [xf[pl.ds(i, PLANE, stride=8), :] for i in range(6)]
    lane = lax.broadcasted_iota(jnp.int32, (PLANE, 128), 1)
    low, high = lane < 32, lane >= 96

    def packed(t0, t1, t2):
        up, half = pltpu.roll(t2, 96, 1), pltpu.roll(t2, 64, 1)
        return jnp.where(high, up, t0), jnp.where(high, half, t1), up, half

    p0, p1, _, last_r = packed(*t[0:3])
    p2, p3, last_i, _ = packed(*t[3:6])
    second = jnp.logical_and(lane >= 32, lane < 64)
    p4 = jnp.where(low, last_r, jnp.where(second, last_i, 0.0))
    xall[v] = jnp.concatenate([p0, p1, p2, p3, p4], axis=1).astype(BF)

    def copy3(d, slot):
        pv = lax.rem(v + d, NVAR)
        return pltpu.make_async_remote_copy(
            src_ref=xall.at[slot],
            dst_ref=xall.at[slot],
            send_sem=s3.at[d],
            recv_sem=r3.at[slot],
            device_id={"var": pv},
            device_id_type=MESH,
        )

    def send3(d, _):
        copy3(d, v).start()
        return 0

    lax.fori_loop(1, NVAR, send3, 0)

    def wait3(d, _):
        copy3(d, lax.rem(v + d, NVAR)).wait_recv()
        return 0

    loads[3].wait()
    loads[4].wait()
    lax.fori_loop(1, NVAR, wait3, 0)
    every = xall[...].reshape(NVAR * CD, 640)

    def combined(g, half):
        re = g[:half, 0:256] - g[half:, 256:512]
        im = g[half:, 0:256] + g[:half, 256:512]
        gr, gi = g[:half, 512:640], g[half:, 512:640]
        which = lax.broadcasted_iota(jnp.int32, (half, 128), 1) < 32
        last = jnp.where(which, gr - pltpu.roll(gi, 96, 1), gr + pltpu.roll(gi, 32, 1))
        return re, im, last, which

    g = jnp.dot(wiv[...].reshape(512, 256), every, preferred_element_type=F32)
    re, im, last, which = combined(g, 256)
    wide_r = jnp.concatenate([bias_r, bias_r], axis=1)
    wide_i = jnp.concatenate([bias_i, bias_i], axis=1)
    hidden = jnp.concatenate(
        [re + wide_r, im + wide_i, last + jnp.where(which, bias_r, bias_i)], axis=1
    )
    hidden = jnp.maximum(hidden, 0.0).astype(BF)
    first = pl.multiple_of(v * CD, CD)
    own = jnp.concatenate([wov[0, pl.ds(first, CD), :], wov[1, pl.ds(first, CD), :]], axis=0)
    g = jnp.dot(own, hidden, preferred_element_type=F32)
    re, im, last, _ = combined(g, CD)
    sel = [lane < 32, lane < 64]
    t2 = jnp.where(
        sel[0],
        pltpu.roll(re[:, 0:128], 32, 1),
        jnp.where(sel[1], pltpu.roll(re[:, 128:256], 64, 1), pltpu.roll(last, 64, 1)),
    )
    t5 = jnp.where(
        sel[0],
        pltpu.roll(im[:, 0:128], 32, 1),
        jnp.where(sel[1], pltpu.roll(im[:, 128:256], 64, 1), pltpu.roll(last, 32, 1)),
    )
    for i, tile in enumerate([re[:, 0:128], re[:, 128:256], t2, im[:, 0:128], im[:, 128:256], t5]):
        mf[pl.ds(i, PLANE, stride=8), :] = tile
    mbuf[...] = mf[...].reshape(PLANE, 8, 128).astype(BF)

    def copy4(d, src, dst, pa, pb):
        return pltpu.make_async_remote_copy(
            src_ref=mbuf.at[src],
            dst_ref=mrecv.at[dst],
            send_sem=s4.at[d],
            recv_sem=r4.at[dst],
            device_id={"lat": pa, "lon": pb},
            device_id_type=MESH,
        )

    def send4(d, _):
        pa, pb = plane(d)
        copy4(d, pa * NLON + pb, me, pa, pb).start()
        return 0

    lax.fori_loop(1, PLANE, send4, 0)
    mrecv[me] = mbuf[me]

    def wait4(d, _):
        pa, pb = plane(d)
        slot = pa * NLON + pb
        copy4(d, slot, slot, pa, pb).wait_recv()
        return 0

    for i in range(5, 8):
        loads[i].wait()
    lax.fori_loop(1, PLANE, wait4, 0)
    modes = mrecv[...].reshape(PLANE * 8, 128)
    back_r = jnp.dot(rv[0:LAT, :], modes, preferred_element_type=F32)
    back_i = jnp.dot(rv[LAT : 2 * LAT, :], modes, preferred_element_type=F32)
    lbv[...] = jnp.concatenate([back_r, back_i], axis=1).astype(BF).reshape(NLAT, RD, 256)

    def copy5(d, slot, pa, pb):
        return pltpu.make_async_remote_copy(
            src_ref=fs.at[d],
            dst_ref=field.at[0, slot],
            send_sem=s5.at[d],
            recv_sem=r5.at[slot],
            device_id={"lat": pa, "lon": pb},
            device_id_type=MESH,
        )

    def block(d):
        pa, pb = plane(d)
        out = jnp.dot(lbv[pa], hv[pb], preferred_element_type=F32)
        act = 0.5 * out * (1.0 + lax.erf(out * (1.0 / math.sqrt(2.0))))
        fs[d] = act.astype(BF)
        return act, pa, pb

    ones = jnp.ones((8, 128), F32)
    weighted = jnp.zeros((8, 128), F32)
    for da in reversed(range(NLAT)):

        def step(d, sums):
            act, pa, pb = block(d)
            copy5(d, me, pa, pb).start()
            return sums[0] + act, sums[1] + act * act

        zero = jnp.zeros((RD, 128), F32)
        if da:
            sums = (zero, zero)
        else:
            act, _, _ = block(0)
            kept = pltpu.make_async_copy(fs.at[0], field.at[0, me], s5.at[0])
            kept.start()
            sums = (act, act * act)
        sums = lax.fori_loop(max(1, da * 8), da * 8 + 8, step, sums)
        pa = lax.rem(a + da, NLAT)
        rowsum = lax.dot_general(
            ones,
            sums[0],
            (((1,), (1,)), ((), ())),
            precision=lax.Precision.HIGHEST,
            preferred_element_type=F32,
        )
        zst[pa, 0:1, 0:RD] = rowsum[0:1] * (1.0 / LON)
        weighted += jnp.dot(
            gv[pa], sums[1], precision=lax.Precision.HIGHEST, preferred_element_type=F32
        )
    total = jnp.sum(weighted, axis=1, keepdims=True)[0:1] * (1.0 / total_area)
    mine = jnp.where(lax.broadcasted_iota(jnp.int32, (1, 128), 1) == me, total, 0.0)
    for band in range(NLAT):
        zst[band, 1:2, :] = mine

    def copy6(d, slot, pa, pb):
        return pltpu.make_async_remote_copy(
            src_ref=zst.at[pa],
            dst_ref=strec.at[slot],
            send_sem=s6.at[d],
            recv_sem=r6.at[slot],
            device_id={"lat": pa, "lon": pb},
            device_id_type=MESH,
        )

    def send6(d, _):
        pa, pb = plane(d)
        copy6(d, me, pa, pb).start()
        return 0

    lax.fori_loop(1, PLANE, send6, 0)
    strec[me] = zst[a]

    def wait6(d, _):
        pa, pb = plane(d)
        copy6(d, pa * NLON + pb, pa, pb).wait_recv()
        return 0

    lax.fori_loop(1, PLANE, wait6, 0)
    gathered = jnp.zeros((1, 128), F32)
    for i in range(CD):
        both = strec[i]
        zonal[i : i + 1, :] = both[0:1, 0:RD]
        gathered += both[1:2, :]
    energy[...] = gathered

    def drain(d, _):
        pa, pb = plane(d)
        slot = pa * NLON + pb
        copy5(d, slot, pa, pb).wait_recv()
        copy1(d, slot, pa, pb).wait_send()
        copy2(d, slot, slot, pa, pb).wait_send()
        copy4(d, slot, slot, pa, pb).wait_send()
        copy5(d, slot, pa, pb).wait_send()
        copy6(d, slot, pa, pb).wait_send()
        return 0

    lax.fori_loop(1, PLANE, drain, 0)

    def drain3(d, _):
        copy3(d, v).wait_send()
        return 0

    lax.fori_loop(1, NVAR, drain3, 0)
    kept.wait()


def body(state, weights_in, bias_in, weights_out):
    *tabs, total_area = tables()
    hbm = pl.BlockSpec(memory_space=pltpu.HBM)
    vmem = pl.BlockSpec(memory_space=pltpu.VMEM)
    dma = pltpu.SemaphoreType.DMA
    field, zonal, energy = pl.pallas_call(
        lambda *refs: kernel(total_area, *refs),
        out_shape=(
            jax.ShapeDtypeStruct((1, CD, RD, ND), BF),
            jax.ShapeDtypeStruct((CD, RD), F32),
            jax.ShapeDtypeStruct((1, 128), F32),
        ),
        in_specs=[hbm] * 7 + [vmem, hbm],
        out_specs=(hbm, vmem, vmem),
        scratch_shapes=[
            pltpu.VMEM((CD, RD, ND), BF),
            pltpu.VMEM((LON, 256), BF),
            pltpu.VMEM((256, 2 * LAT), BF),
            pltpu.VMEM((2 * LAT, 256), BF),
            pltpu.VMEM((NLON, 256, ND), BF),
            pltpu.VMEM((NLAT, 8, RD), F32),
            pltpu.VMEM((2, 256, 256), BF),
            pltpu.VMEM((2, 256, 256), BF),
            pltpu.VMEM((128, 256), F32),
            pltpu.VMEM((PLANE, RD, ND), BF),
            pltpu.VMEM((NLAT, RD, 256), BF),
            pltpu.VMEM((PLANE, 8, 128), BF),
            pltpu.VMEM((PLANE, 8, 128), BF),
            pltpu.VMEM((PLANE * 8, 128), F32),
            pltpu.VMEM((NVAR, CD, 640), BF),
            pltpu.VMEM((PLANE * 8, 128), F32),
            pltpu.VMEM((PLANE, 8, 128), BF),
            pltpu.VMEM((PLANE, 8, 128), BF),
            pltpu.VMEM((NLAT, RD, 256), BF),
            pltpu.VMEM((PLANE, RD, ND), BF),
            pltpu.VMEM((NLAT, 2, 128), F32),
            pltpu.VMEM((PLANE, 2, 128), F32),
            dma((8,)),
        ]
        + [dma((PLANE,)), dma((PLANE,))] * 2
        + [dma((NVAR,)), dma((NVAR,))]
        + [dma((PLANE,)), dma((PLANE,))] * 3,
        compiler_params=pltpu.CompilerParams(
            collective_id=0, has_side_effects=True, vmem_limit_bytes=32 * 1024 * 1024
        ),
        name="spectral_layer",
    )(state, *(jnp.asarray(t) for t in tabs), weights_in, bias_in, weights_out)
    return field, zonal.reshape(1, CD, RD), energy[0, :CD]


def solution(mesh):
    return jax.shard_map(
        body,
        mesh=mesh,
        in_specs=(P(None, "var", "lat", "lon"), P(), P(), P()),
        out_specs=(P(None, "var", "lat", "lon"), P(None, "var", "lat"), P("var")),
        check_vma=False,
    )
```

```python
import math

import jax
import jax.numpy as jnp
import numpy as np
from jax import lax
from jax.experimental import pallas as pl
from jax.experimental.pallas import tpu as pltpu
from jax.sharding import PartitionSpec as P

LAT = 384
LON = 1024
MLAT = 96
MLON = 96
NVAR = 8
NLAT = 4
NLON = 8
PLANE = NLAT * NLON
CD = 32
RD = LAT // NLAT
ND = LON // NLON
JO = MLAT // PLANE
MESH = pl.DeviceIdType.MESH
TAIL_AT = 0.23
TAIL = (
    0.09190782232377631,
    0.08914107185889676,
    0.10610870974692016,
    -0.0007481814870291388,
    0.25362340835459335,
    -0.23501017104744312,
    0.2688627946887361,
    -0.0738853870258165,
)
BF = jnp.bfloat16
F32 = jnp.float32


def ring(d):
    return min(d, 4 - d)


CHIPS = sorted(((i, j) for i in range(4) for j in range(4) if i or j), key=lambda c: -ring(c[0]) - ring(c[1]))
PEERS = [(i, j, c) for i, j in CHIPS for c in range(2)] + [(0, 0, 1)]


def gelu(x):
    size = jnp.abs(x)
    t = 1.0 / (1.0 + TAIL_AT * size)
    poly = TAIL[-1]
    for c in TAIL[-2::-1]:
        poly = poly * t + c
    tail = (size * t) * poly * jnp.exp2((x * x) * (-0.5 / math.log(2.0)))
    return jnp.maximum(x, 0.0) - tail


def tables():
    k = np.arange(MLON)
    n = np.arange(LON)
    angle = 2.0 * np.pi / LON * ((n[:, None] * k[None, :]) % LON)
    scale = 1.0 / math.sqrt(LAT * LON)
    etab = np.zeros((LON, 256), np.float32)
    etab[:, :MLON] = np.cos(angle) * scale
    etab[:, 128 : 128 + MLON] = -np.sin(angle) * scale
    weight = np.where(k == 0, 1.0, 2.0)[:, None] * scale
    full = np.zeros((256, LON), np.float32)
    full[:MLON] = weight * np.cos(angle.T)
    full[128 : 128 + MLON] = -weight * np.sin(angle.T)
    htab = full.reshape(256, 4, 2 * ND).transpose(1, 0, 2)
    r = np.arange(LAT)
    freqs = np.arange(MLAT) - MLAT // 2
    turn = 2.0 * np.pi / LAT * np.mod(freqs[:, None] * r[None, :], LAT)
    cosine, sine = np.cos(turn), np.sin(turn)
    forward = np.zeros((PLANE, 8, 2, LAT), np.float32)
    forward[:, 0:3, 0] = cosine.reshape(PLANE, JO, LAT)
    forward[:, 0:3, 1] = sine.reshape(PLANE, JO, LAT)
    forward[:, 3:6, 0] = -sine.reshape(PLANE, JO, LAT)
    forward[:, 3:6, 1] = cosine.reshape(PLANE, JO, LAT)
    qtab = forward.reshape(PLANE * 8, 2 * LAT)
    rtab = qtab.T
    area = np.cos(np.pi * ((r + 0.5) / LAT - 0.5))
    gtab = np.broadcast_to(area.reshape(NLAT, 1, RD), (NLAT, 8, RD))
    bf = lambda t: np.ascontiguousarray(t).astype(jnp.bfloat16)
    return (
        bf(etab),
        bf(qtab),
        bf(rtab),
        bf(htab),
        np.ascontiguousarray(gtab).astype(np.float32),
        float(LON * area.sum()),
    )


SCOPES = []


def scope(name):
    while SCOPES:
        SCOPES.pop().__exit__(None, None, None)
    if name:
        SCOPES.append(jax.named_scope(name))
        SCOPES[-1].__enter__()


def kernel(
    total_area,
    state,
    etab,
    qtab,
    rtab,
    htab,
    gtab,
    win,
    bias,
    wout,
    field,
    stats,
    st,
    ev,
    qv,
    rv,
    hv,
    gv,
    wiv,
    wov,
    bcol,
    xin,
    lv,
    sbuf,
    srecv,
    xf,
    xall,
    mf,
    mbuf,
    mrecv,
    lbv,
    fs,
    acc,
    acc2,
    zst,
    load_sem,
    s1,
    r1,
    s2,
    r2,
    s3,
    r3,
    s4,
    r4,
    s5,
    r5,
    s6,
    r6,
):
    v = lax.axis_index("var")
    a = lax.axis_index("lat")
    b = lax.axis_index("lon")
    y, core = lax.div(b, 2), lax.rem(b, 2)

    def slot_of(pa, py, pc):
        return pc * 16 + pa * 4 + py

    me = slot_of(a, y, core)
    lats = [lax.rem(a + i, 4) for i in range(4)]
    ys = [lax.rem(y + i, 4) for i in range(4)]
    cores = [core, 1 - core]

    def plane(peer):
        i, j, c = peer
        pa, py, pc = lats[i], ys[j], cores[c]
        return {"lat": pa, "lon": py * 2 + pc}, slot_of(pa, py, pc)

    def at_slot(slot):
        pa, py, pc = lax.div(lax.rem(slot, 16), 4), lax.rem(slot, 4), lax.div(slot, 16)
        return {"lat": pa, "lon": py * 2 + pc}

    scope("greet")
    barrier = pltpu.get_barrier_semaphore()
    for peer in PEERS:
        pl.semaphore_signal(barrier, inc=1, device_id=plane(peer)[0], device_id_type=MESH)
    far = (4, 3, 5, 2, 6, 1, 7)
    vars_ = {d: lax.rem(v + d, NVAR) for d in far}
    for d in far:
        pl.semaphore_signal(barrier, inc=1, device_id={"var": vars_[d]}, device_id_type=MESH)

    loads = [
        pltpu.make_async_copy(src, dst, load_sem.at[i])
        for i, (src, dst) in enumerate(
            [
                (state.at[0], st),
                (bias, bcol.at[0:2]),
                (etab, ev),
                (qtab, qv),
                (win, wiv),
                (wout, wov),
                (rtab, rv),
                (htab, hv),
                (gtab, gv),
            ]
        )
    ]
    for load in loads:
        load.start()
    mf[...] = jnp.zeros_like(mf)
    zst[...] = jnp.zeros_like(zst)
    acc[...] = jnp.zeros_like(acc)
    acc2[...] = jnp.zeros_like(acc2)
    scope("barrier")
    loads[0].wait()
    pl.semaphore_wait(barrier, PLANE - 1 + NVAR - 1)

    def all_but_me(first, last, wait):
        def step(slot, _):
            @pl.when(slot != me)
            def _():
                wait(slot)

            return 0

        lax.fori_loop(first, last, step, 0)

    def copy1(src, dst, to):
        return pltpu.make_async_remote_copy(
            src_ref=st.at[src],
            dst_ref=xin.at[dst],
            send_sem=s1.at[src],
            recv_sem=r1.at[dst],
            device_id=to,
            device_id_type=MESH,
        )

    scope("send1")
    for pc in range(2):
        for i, j in [*CHIPS, (0, 0)]:
            slot = slot_of(lats[i], ys[j], pc)

            def start(i=i, j=j, slot=slot):
                copy1(slot, me, {"lat": lats[i], "lon": ys[j] * 2 + pc}).start()

            if i or j:
                start()
            else:
                pl.when(core != pc)(start)
    xin[me] = st[me]
    scope("wait1")
    loads[1].wait()
    turned = jnp.transpose(bcol[...])
    bias_r = jnp.broadcast_to(turned[:, 0:1], (256, 128))
    bias_i = jnp.broadcast_to(turned[:, 1:2], (256, 128))
    loads[2].wait()
    for da in (0, 1, 3, 2):
        pa = lats[da]

        def wait1(i, _):
            slot = lax.div(i, 4) * 16 + pa * 4 + lax.rem(i, 4)

            @pl.when(slot != me)
            def _():
                copy1(slot, slot, at_slot(slot)).wait_recv()

            return 0

        lax.fori_loop(0, NLON, wait1, 0)
        rows = jnp.concatenate([xin[(i % 2) * 16 + pa * 4 + i // 2] for i in range(NLON)], axis=1)
        lv[pa] = jnp.dot(rows, ev[...], preferred_element_type=F32).astype(BF)

    scope("fwd")
    loads[3].wait()
    lon = lv[...].reshape(LAT, 256)
    spec = jnp.dot(qv[:, 0:LAT], lon[:, 0:128], preferred_element_type=F32)
    spec += jnp.dot(qv[:, LAT : 2 * LAT], lon[:, 128:256], preferred_element_type=F32)
    sbuf[...] = spec.reshape(PLANE, 8, 128).astype(BF)

    def copy2(src, dst, to):
        return pltpu.make_async_remote_copy(
            src_ref=sbuf.at[src],
            dst_ref=srecv.at[dst],
            send_sem=s2.at[src],
            recv_sem=r2.at[dst],
            device_id=to,
            device_id_type=MESH,
        )

    scope("send2")
    for peer in PEERS:
        to, slot = plane(peer)
        copy2(slot, me, to).start()
    srecv[me] = sbuf[me]

    lane = lax.broadcasted_iota(jnp.int32, (16, 128), 1)
    low, high = lane < 32, lane >= 96
    second = jnp.logical_and(lane >= 32, lane < 64)

    def packed(t0, t1, t2):
        up, half = pltpu.roll(t2, 96, 1), pltpu.roll(t2, 64, 1)
        return jnp.where(high, up, t0), jnp.where(high, half, t1), up, half

    def copy3(half, d, slot):
        part = xall.at[slot, pl.ds(half * 16, 16)]
        return pltpu.make_async_remote_copy(
            src_ref=part,
            dst_ref=part,
            send_sem=s3.at[half, d],
            recv_sem=r3.at[half, slot],
            device_id={"var": vars_[d]},
            device_id_type=MESH,
        )

    for half in range(2):
        scope(f"wait2_{half}")
        all_but_me(half * 16, half * 16 + 16, lambda slot: copy2(slot, slot, at_slot(slot)).wait_recv())
        scope(f"pack_{half}")
        xf[...] = srecv[half * 16 : half * 16 + 16].astype(F32).reshape(128, 128)
        t = [xf[pl.ds(i, 16, stride=8), :] for i in range(6)]
        p0, p1, _, last_r = packed(*t[0:3])
        p2, p3, last_i, _ = packed(*t[3:6])
        p4 = jnp.where(low, last_r, jnp.where(second, last_i, 0.0))
        xall[v, half * 16 : half * 16 + 16] = jnp.concatenate([p0, p1, p2, p3, p4], axis=1).astype(BF)
        for d in far:
            copy3(half, d, v).start()

    scope("wait3")
    loads[4].wait()
    loads[5].wait()
    for half in range(2):
        for d in reversed(far):
            copy3(half, d, vars_[d]).wait_recv()
    scope("mix")
    every = xall[...].reshape(NVAR * CD, 640)

    def combined(g, half):
        re = g[:half, 0:256] - g[half:, 256:512]
        im = g[half:, 0:256] + g[:half, 256:512]
        gr, gi = g[:half, 512:640], g[half:, 512:640]
        which = lax.broadcasted_iota(jnp.int32, (half, 128), 1) < 32
        last = jnp.where(which, gr - pltpu.roll(gi, 96, 1), gr + pltpu.roll(gi, 32, 1))
        return re, im, last, which

    g = jnp.dot(wiv[...].reshape(512, 256), every, preferred_element_type=F32)
    re, im, last, which = combined(g, 256)
    wide_r = jnp.concatenate([bias_r, bias_r], axis=1)
    wide_i = jnp.concatenate([bias_i, bias_i], axis=1)
    hidden = jnp.concatenate(
        [re + wide_r, im + wide_i, last + jnp.where(which, bias_r, bias_i)], axis=1
    )
    hidden = jnp.maximum(hidden, 0.0).astype(BF)
    first = pl.multiple_of(v * CD, CD)
    own = jnp.concatenate([wov[0, pl.ds(first, CD), :], wov[1, pl.ds(first, CD), :]], axis=0)
    g = jnp.dot(own, hidden, preferred_element_type=F32)
    re, im, last, _ = combined(g, CD)
    lane = lax.broadcasted_iota(jnp.int32, (CD, 128), 1)
    sel = [lane < 32, lane < 64]
    t2 = jnp.where(
        sel[0],
        pltpu.roll(re[:, 0:128], 32, 1),
        jnp.where(sel[1], pltpu.roll(re[:, 128:256], 64, 1), pltpu.roll(last, 64, 1)),
    )
    t5 = jnp.where(
        sel[0],
        pltpu.roll(im[:, 0:128], 32, 1),
        jnp.where(sel[1], pltpu.roll(im[:, 128:256], 64, 1), pltpu.roll(last, 32, 1)),
    )
    for i, tile in enumerate([re[:, 0:128], re[:, 128:256], t2, im[:, 0:128], im[:, 128:256], t5]):
        mf[pl.ds(i, PLANE, stride=8), :] = tile
    mbuf[...] = mf[...].reshape(PLANE, 8, 128).astype(BF)

    def copy4(src, dst, to):
        return pltpu.make_async_remote_copy(
            src_ref=mbuf.at[src],
            dst_ref=mrecv.at[dst],
            send_sem=s4.at[src],
            recv_sem=r4.at[dst],
            device_id=to,
            device_id_type=MESH,
        )

    scope("send4")
    for peer in PEERS:
        to, slot = plane(peer)
        copy4(slot, me, to).start()
    mrecv[me] = mbuf[me]
    scope("wait4")
    for load in loads[6:]:
        load.wait()
    all_but_me(0, PLANE, lambda slot: copy4(slot, slot, at_slot(slot)).wait_recv())
    scope("back")
    modes = mrecv[...].reshape(PLANE * 8, 128)
    back_r = jnp.dot(rv[0:LAT, :], modes, preferred_element_type=F32)
    back_i = jnp.dot(rv[LAT : 2 * LAT, :], modes, preferred_element_type=F32)
    lbv[...] = jnp.concatenate([back_r, back_i], axis=1).astype(BF).reshape(NLAT, RD, 256)

    def copy5(src, dst, to):
        return pltpu.make_async_remote_copy(
            src_ref=fs.at[src],
            dst_ref=field.at[0, dst],
            send_sem=s5.at[src],
            recv_sem=r5.at[dst],
            device_id=to,
            device_id_type=MESH,
        )

    def chip(i, j):
        pa, py = lats[i], ys[j]
        act = gelu(jnp.dot(lbv[pa], hv[py], preferred_element_type=F32))
        fs[slot_of(pa, py, 0)] = act[:, 0:128].astype(BF)
        fs[slot_of(pa, py, 1)] = act[:, 128:256].astype(BF)
        acc[pa] += act[:, 0:128] + act[:, 128:256]
        square = act * act
        acc2[pa] += square[:, 0:128] + square[:, 128:256]

    def send5(peer):
        to, slot = plane(peer)
        copy5(slot, me, to).start()

    scope("gelu")
    near = [c for c in CHIPS if ring(c[0]) + ring(c[1]) == 1]
    for c in CHIPS:
        chip(*c)
        if c not in near:
            send5((*c, 0))
            send5((*c, 1))
    chip(0, 0)
    scope("stats")
    ones = jnp.ones((8, 128), F32)
    weighted = jnp.zeros((8, 128), F32)
    for band in range(NLAT):
        rowsum = lax.dot_general(
            ones,
            acc[band],
            (((1,), (1,)), ((), ())),
            precision=lax.Precision.HIGHEST,
            preferred_element_type=F32,
        )
        zst[band, 0:1, 0:RD] = rowsum[0:1] * (1.0 / LON)
        weighted += jnp.dot(
            gv[band], acc2[band], precision=lax.Precision.HIGHEST, preferred_element_type=F32
        )
    total = jnp.sum(weighted, axis=1, keepdims=True)[0:1] * (1.0 / total_area)
    mine = jnp.where(lax.broadcasted_iota(jnp.int32, (1, 128), 1) == me, total, 0.0)
    for band in range(NLAT):
        zst[band, 1:2, :] = mine

    def copy6(src, dst, band, to):
        return pltpu.make_async_remote_copy(
            src_ref=zst.at[band],
            dst_ref=stats.at[dst],
            send_sem=s6.at[src],
            recv_sem=r6.at[dst],
            device_id=to,
            device_id_type=MESH,
        )

    scope("send6")
    for peer in PEERS:
        to, slot = plane(peer)
        copy6(slot, me, lats[peer[0]], to).start()
    for c in near:
        send5((*c, 0))
        send5((*c, 1))
    send5((0, 0, 1))
    field[0, me] = fs[me]
    stats[me] = zst[a]
    scope("wait5")

    def ended(slot):
        to = at_slot(slot)
        copy1(slot, slot, to).wait_send()
        copy2(slot, slot, to).wait_send()
        copy4(slot, slot, to).wait_send()

    all_but_me(0, PLANE, ended)
    for half in range(2):
        for d in far:
            copy3(half, d, v).wait_send()

    def arrived(slot):
        to = at_slot(slot)
        copy5(slot, slot, to).wait_send()
        copy6(slot, slot, a, to).wait_send()
        copy5(slot, slot, to).wait_recv()
        copy6(slot, slot, a, to).wait_recv()

    all_but_me(0, PLANE, arrived)
    scope(None)


def finish(field, stats, out, zonal, energy, zv, evec, sems):
    big = pltpu.make_async_copy(field, out, sems.at[0])
    big.start()
    gathered = jnp.zeros((1, 128), F32)
    for i in range(CD):
        both = stats[i]
        zv[0, i : i + 1, :] = both[0:1, 0:RD]
        gathered += both[1:2, :]
    evec[...] = gathered[0, 0:CD]
    small = pltpu.make_async_copy(zv, zonal, sems.at[1])
    small.start()
    other = pltpu.make_async_copy(evec, energy, sems.at[2])
    other.start()
    big.wait()
    small.wait()
    other.wait()


def body(state, weights_in, bias_in, weights_out):
    *tabs, total_area = tables()
    hbm = pl.BlockSpec(memory_space=pltpu.HBM)
    vmem = pl.BlockSpec(memory_space=pltpu.VMEM)
    dma = pltpu.SemaphoreType.DMA
    operands = (state, *(jnp.asarray(t) for t in tabs), weights_in, bias_in, weights_out)
    field, stats = pl.pallas_call(
        lambda *refs: kernel(total_area, *refs),
        out_shape=(
            jax.ShapeDtypeStruct((1, CD, RD, ND), BF),
            jax.ShapeDtypeStruct((PLANE, 2, 128), F32),
        ),
        in_specs=[hbm] * 9,
        out_specs=(vmem, vmem),
        scratch_shapes=[
            pltpu.VMEM((CD, RD, ND), BF),
            pltpu.VMEM((LON, 256), BF),
            pltpu.VMEM((256, 2 * LAT), BF),
            pltpu.VMEM((2 * LAT, 256), BF),
            pltpu.VMEM((4, 256, 256), BF),
            pltpu.VMEM((NLAT, 8, RD), F32),
            pltpu.VMEM((2, 256, 256), BF),
            pltpu.VMEM((2, 256, 256), BF),
            pltpu.VMEM((128, 256), F32),
            pltpu.VMEM((PLANE, RD, ND), BF),
            pltpu.VMEM((NLAT, RD, 256), BF),
            pltpu.VMEM((PLANE, 8, 128), BF),
            pltpu.VMEM((PLANE, 8, 128), BF),
            pltpu.VMEM((128, 128), F32),
            pltpu.VMEM((NVAR, CD, 640), BF),
            pltpu.VMEM((PLANE * 8, 128), F32),
            pltpu.VMEM((PLANE, 8, 128), BF),
            pltpu.VMEM((PLANE, 8, 128), BF),
            pltpu.VMEM((NLAT, RD, 256), BF),
            pltpu.VMEM((PLANE, RD, ND), BF),
            pltpu.VMEM((NLAT, RD, 128), F32),
            pltpu.VMEM((NLAT, RD, 128), F32),
            pltpu.VMEM((NLAT, 2, 128), F32),
            dma((9,)),
        ]
        + [dma((PLANE,)), dma((PLANE,))] * 2
        + [dma((2, NVAR)), dma((2, NVAR))]
        + [dma((PLANE,)), dma((PLANE,))] * 3,
        compiler_params=pltpu.CompilerParams(
            collective_id=0, has_side_effects=True, vmem_limit_bytes=32 * 1024 * 1024
        ),
        name="spectral_layer",
    )(*(pltpu.with_memory_space_constraint(x, pltpu.HBM) for x in operands))
    return pl.pallas_call(
        finish,
        out_shape=(
            jax.ShapeDtypeStruct((1, CD, RD, ND), BF),
            jax.ShapeDtypeStruct((1, CD, RD), F32),
            jax.ShapeDtypeStruct((CD,), F32),
        ),
        in_specs=[vmem, vmem],
        out_specs=(hbm, hbm, hbm),
        scratch_shapes=[
            pltpu.VMEM((1, CD, RD), F32),
            pltpu.VMEM((CD,), F32),
            dma((3,)),
        ],
        compiler_params=pltpu.CompilerParams(vmem_limit_bytes=8 * 1024 * 1024),
        name="finish",
    )(field, stats)


def solution(mesh):
    return jax.shard_map(
        body,
        mesh=mesh,
        in_specs=(P(None, "var", "lat", "lon"), P(), P(), P()),
        out_specs=(P(None, "var", "lat", "lon"), P(None, "var", "lat"), P("var")),
        check_vma=False,
    )
```

```python
import math

import jax
import jax.numpy as jnp
import numpy as np
from jax import lax
from jax.experimental import pallas as pl
from jax.experimental.pallas import tpu as pltpu
from jax.sharding import PartitionSpec as P

LAT = 384
LON = 1024
MLAT = 96
MLON = 96
NVAR = 8
NLAT = 4
NLON = 8
PLANE = NLAT * NLON
CD = 32
RD = LAT // NLAT
ND = LON // NLON
JO = MLAT // PLANE
MESH = pl.DeviceIdType.MESH
TAIL_AT = 0.23
TAIL = (
    0.09190782232377631,
    0.08914107185889676,
    0.10610870974692016,
    -0.0007481814870291388,
    0.25362340835459335,
    -0.23501017104744312,
    0.2688627946887361,
    -0.0738853870258165,
)
BF = jnp.bfloat16
F32 = jnp.float32


def ring(d):
    return min(d, 4 - d)


CHIPS = sorted(((i, j) for i in range(4) for j in range(4) if i or j), key=lambda c: -ring(c[0]) - ring(c[1]))
PEERS = [(i, j, c) for i, j in CHIPS for c in range(2)] + [(0, 0, 1)]


def gelu(x):
    size = jnp.abs(x)
    t = 1.0 / (1.0 + TAIL_AT * size)
    poly = TAIL[-1]
    for c in TAIL[-2::-1]:
        poly = poly * t + c
    tail = (size * t) * poly * jnp.exp2((x * x) * (-0.5 / math.log(2.0)))
    return jnp.maximum(x, 0.0) - tail


def tables():
    k = np.arange(MLON)
    n = np.arange(LON)
    angle = 2.0 * np.pi / LON * ((n[:, None] * k[None, :]) % LON)
    scale = 1.0 / math.sqrt(LAT * LON)
    etab = np.zeros((LON, 256), np.float32)
    etab[:, :MLON] = np.cos(angle) * scale
    etab[:, 128 : 128 + MLON] = -np.sin(angle) * scale
    weight = np.where(k == 0, 1.0, 2.0)[:, None] * scale
    full = np.zeros((256, LON), np.float32)
    full[:MLON] = weight * np.cos(angle.T)
    full[128 : 128 + MLON] = -weight * np.sin(angle.T)
    htab = full.reshape(256, 4, 2 * ND).transpose(1, 0, 2)
    r = np.arange(LAT)
    freqs = np.arange(MLAT) - MLAT // 2
    turn = 2.0 * np.pi / LAT * np.mod(freqs[:, None] * r[None, :], LAT)
    cosine, sine = np.cos(turn), np.sin(turn)
    forward = np.zeros((PLANE, 8, 2, LAT), np.float32)
    forward[:, 0:3, 0] = cosine.reshape(PLANE, JO, LAT)
    forward[:, 0:3, 1] = sine.reshape(PLANE, JO, LAT)
    forward[:, 3:6, 0] = -sine.reshape(PLANE, JO, LAT)
    forward[:, 3:6, 1] = cosine.reshape(PLANE, JO, LAT)
    qtab = forward.reshape(PLANE * 8, 2 * LAT)
    rtab = qtab.T
    area = np.cos(np.pi * ((r + 0.5) / LAT - 0.5))
    gtab = np.broadcast_to(area.reshape(NLAT, 1, RD), (NLAT, 8, RD))
    bf = lambda t: np.ascontiguousarray(t).astype(jnp.bfloat16)
    return (
        bf(etab),
        bf(qtab),
        bf(rtab),
        bf(htab),
        np.ascontiguousarray(gtab).astype(np.float32),
        float(LON * area.sum()),
    )


SCOPES = []


def scope(name):
    while SCOPES:
        SCOPES.pop().__exit__(None, None, None)
    if name:
        SCOPES.append(jax.named_scope(name))
        SCOPES[-1].__enter__()


def kernel(
    total_area,
    state,
    etab,
    qtab,
    rtab,
    htab,
    gtab,
    win,
    bias,
    wout,
    field,
    stats,
    st,
    ev,
    qv,
    rv,
    hv,
    gv,
    wiv,
    wov,
    bcol,
    xin,
    lv,
    sbuf,
    srecv,
    xf,
    xall,
    mf,
    mbuf,
    mrecv,
    lbv,
    fs,
    acc,
    acc2,
    zst,
    load_sem,
    s1,
    r1,
    s2,
    r2,
    s3,
    r3,
    s4,
    r4,
    s5,
    r5,
    s6,
    r6,
):
    v = lax.axis_index("var")
    a = lax.axis_index("lat")
    b = lax.axis_index("lon")
    y, core = lax.div(b, 2), lax.rem(b, 2)

    def slot_of(pa, py, pc):
        return pc * 16 + pa * 4 + py

    me = slot_of(a, y, core)
    lats = [lax.rem(a + i, 4) for i in range(4)]
    ys = [lax.rem(y + i, 4) for i in range(4)]
    cores = [core, 1 - core]

    def plane(peer):
        i, j, c = peer
        pa, py, pc = lats[i], ys[j], cores[c]
        return {"lat": pa, "lon": py * 2 + pc}, slot_of(pa, py, pc)

    loads = [
        pltpu.make_async_copy(src, dst, load_sem.at[i])
        for i, (src, dst) in enumerate(
            [
                (state.at[0], st),
                (bias, bcol.at[0:2]),
                (etab, ev),
                (qtab, qv),
                (win, wiv),
                (wout, wov),
                (rtab, rv),
                (htab, hv),
                (gtab, gv),
            ]
        )
    ]
    loads[0].start()
    scope("greet")
    barrier = pltpu.get_barrier_semaphore()
    for peer in PEERS:
        pl.semaphore_signal(barrier, inc=1, device_id=plane(peer)[0], device_id_type=MESH)
    far = (4, 3, 5, 2, 6, 1, 7)
    vars_ = {d: lax.rem(v + d, NVAR) for d in far}
    for d in far:
        pl.semaphore_signal(barrier, inc=1, device_id={"var": vars_[d]}, device_id_type=MESH)

    for load in loads[1:]:
        load.start()
    mf[...] = jnp.zeros_like(mf)
    zst[...] = jnp.zeros_like(zst)
    acc[...] = jnp.zeros_like(acc)
    acc2[...] = jnp.zeros_like(acc2)
    scope("barrier")
    loads[0].wait()
    pl.semaphore_wait(barrier, PLANE - 1 + NVAR - 1)

    def whole(ref, sem):
        some = ref.at[pl.ds(0, PLANE - 1)]
        pltpu.make_async_copy(some, some, sem.at[0]).wait()

    def copy1(src, dst, band, to):
        return pltpu.make_async_remote_copy(
            src_ref=st.at[src],
            dst_ref=xin.at[dst],
            send_sem=s1.at[0],
            recv_sem=r1.at[band],
            device_id=to,
            device_id_type=MESH,
        )

    scope("send1")
    for peer in PEERS:
        to, slot = plane(peer)
        copy1(slot, me, a, to).start()
    xin[me] = st[me]
    scope("wait1")
    loads[1].wait()
    turned = jnp.transpose(bcol[...])
    bias_r = jnp.broadcast_to(turned[:, 0:1], (256, 128))
    bias_i = jnp.broadcast_to(turned[:, 1:2], (256, 128))
    loads[2].wait()
    for da in (0, 1, 3, 2):
        pa = lats[da]

        some = xin.at[pl.ds(0, NLON if da else NLON - 1)]
        pltpu.make_async_copy(some, some, r1.at[pa]).wait()
        rows = jnp.concatenate([xin[(i % 2) * 16 + pa * 4 + i // 2] for i in range(NLON)], axis=1)
        lv[pa] = jnp.dot(rows, ev[...], preferred_element_type=F32).astype(BF)

    scope("fwd")
    loads[3].wait()
    lon = lv[...].reshape(LAT, 256)
    spec = jnp.dot(qv[:, 0:LAT], lon[:, 0:128], preferred_element_type=F32)
    spec += jnp.dot(qv[:, LAT : 2 * LAT], lon[:, 128:256], preferred_element_type=F32)
    sbuf[...] = spec.reshape(PLANE, 8, 128).astype(BF)

    def copy2(src, dst, to):
        return pltpu.make_async_remote_copy(
            src_ref=sbuf.at[src],
            dst_ref=srecv.at[dst],
            send_sem=s2.at[0],
            recv_sem=r2.at[0],
            device_id=to,
            device_id_type=MESH,
        )

    scope("send2")
    for peer in PEERS:
        to, slot = plane(peer)
        copy2(slot, me, to).start()
    srecv[me] = sbuf[me]

    scope("wait2")
    whole(srecv, r2)
    scope("pack")
    xf[...] = srecv[...].astype(F32).reshape(PLANE * 8, 128)
    t = [xf[pl.ds(i, PLANE, stride=8), :] for i in range(6)]
    lane = lax.broadcasted_iota(jnp.int32, (PLANE, 128), 1)
    low, high = lane < 32, lane >= 96
    second = jnp.logical_and(lane >= 32, lane < 64)

    def packed(t0, t1, t2):
        up, half = pltpu.roll(t2, 96, 1), pltpu.roll(t2, 64, 1)
        return jnp.where(high, up, t0), jnp.where(high, half, t1), up, half

    p0, p1, _, last_r = packed(*t[0:3])
    p2, p3, last_i, _ = packed(*t[3:6])
    p4 = jnp.where(low, last_r, jnp.where(second, last_i, 0.0))
    xall[v] = jnp.concatenate([p0, p1, p2, p3, p4], axis=1).astype(BF)
    for d in far:
        pltpu.make_async_remote_copy(
            src_ref=xall.at[v],
            dst_ref=xall.at[v],
            send_sem=s3.at[0],
            recv_sem=r3.at[0],
            device_id={"var": vars_[d]},
            device_id_type=MESH,
        ).start()

    scope("wait3")
    loads[4].wait()
    loads[5].wait()
    others = xall.at[pl.ds(0, NVAR - 1)]
    pltpu.make_async_copy(others, others, r3.at[0]).wait()
    scope("mix")
    every = xall[...].reshape(NVAR * CD, 640)

    def combined(g, half):
        re = g[:half, 0:256] - g[half:, 256:512]
        im = g[half:, 0:256] + g[:half, 256:512]
        gr, gi = g[:half, 512:640], g[half:, 512:640]
        which = lax.broadcasted_iota(jnp.int32, (half, 128), 1) < 32
        last = jnp.where(which, gr - pltpu.roll(gi, 96, 1), gr + pltpu.roll(gi, 32, 1))
        return re, im, last, which

    g = jnp.dot(wiv[...].reshape(512, 256), every, preferred_element_type=F32)
    re, im, last, which = combined(g, 256)
    wide_r = jnp.concatenate([bias_r, bias_r], axis=1)
    wide_i = jnp.concatenate([bias_i, bias_i], axis=1)
    hidden = jnp.concatenate(
        [re + wide_r, im + wide_i, last + jnp.where(which, bias_r, bias_i)], axis=1
    )
    hidden = jnp.maximum(hidden, 0.0).astype(BF)
    first = pl.multiple_of(v * CD, CD)
    own = jnp.concatenate([wov[0, pl.ds(first, CD), :], wov[1, pl.ds(first, CD), :]], axis=0)
    g = jnp.dot(own, hidden, preferred_element_type=F32)
    re, im, last, _ = combined(g, CD)
    lane = lax.broadcasted_iota(jnp.int32, (CD, 128), 1)
    sel = [lane < 32, lane < 64]
    t2 = jnp.where(
        sel[0],
        pltpu.roll(re[:, 0:128], 32, 1),
        jnp.where(sel[1], pltpu.roll(re[:, 128:256], 64, 1), pltpu.roll(last, 64, 1)),
    )
    t5 = jnp.where(
        sel[0],
        pltpu.roll(im[:, 0:128], 32, 1),
        jnp.where(sel[1], pltpu.roll(im[:, 128:256], 64, 1), pltpu.roll(last, 32, 1)),
    )
    for i, tile in enumerate([re[:, 0:128], re[:, 128:256], t2, im[:, 0:128], im[:, 128:256], t5]):
        mf[pl.ds(i, PLANE, stride=8), :] = tile
    mbuf[...] = mf[...].reshape(PLANE, 8, 128).astype(BF)

    def copy4(src, dst, to):
        return pltpu.make_async_remote_copy(
            src_ref=mbuf.at[src],
            dst_ref=mrecv.at[dst],
            send_sem=s4.at[0],
            recv_sem=r4.at[0],
            device_id=to,
            device_id_type=MESH,
        )

    scope("send4")
    for peer in PEERS:
        to, slot = plane(peer)
        copy4(slot, me, to).start()
    mrecv[me] = mbuf[me]
    scope("wait4")
    for load in loads[6:]:
        load.wait()
    whole(mrecv, r4)
    scope("back")
    modes = mrecv[...].reshape(PLANE * 8, 128)
    back_r = jnp.dot(rv[0:LAT, :], modes, preferred_element_type=F32)
    back_i = jnp.dot(rv[LAT : 2 * LAT, :], modes, preferred_element_type=F32)
    lbv[...] = jnp.concatenate([back_r, back_i], axis=1).astype(BF).reshape(NLAT, RD, 256)

    def copy5(src, dst, to):
        return pltpu.make_async_remote_copy(
            src_ref=fs.at[src],
            dst_ref=field.at[0, dst],
            send_sem=s5.at[0],
            recv_sem=r5.at[0],
            device_id=to,
            device_id_type=MESH,
        )

    def chip(i, j):
        pa, py = lats[i], ys[j]
        act = gelu(jnp.dot(lbv[pa], hv[py], preferred_element_type=F32))
        fs[slot_of(pa, py, 0)] = act[:, 0:128].astype(BF)
        fs[slot_of(pa, py, 1)] = act[:, 128:256].astype(BF)
        acc[pa] += act[:, 0:128] + act[:, 128:256]
        square = act * act
        acc2[pa] += square[:, 0:128] + square[:, 128:256]

    def send5(peer):
        to, slot = plane(peer)
        copy5(slot, me, to).start()

    scope("gelu")
    near = [c for c in CHIPS if ring(c[0]) + ring(c[1]) <= 2]
    for c in CHIPS:
        chip(*c)
        if c not in near:
            send5((*c, 0))
            send5((*c, 1))
    chip(0, 0)
    scope("stats")
    ones = jnp.ones((8, 128), F32)
    weighted = jnp.zeros((8, 128), F32)
    for band in range(NLAT):
        rowsum = lax.dot_general(
            ones,
            acc[band],
            (((1,), (1,)), ((), ())),
            precision=lax.Precision.HIGHEST,
            preferred_element_type=F32,
        )
        zst[band, 0:1, 0:RD] = rowsum[0:1] * (1.0 / LON)
        weighted += jnp.dot(
            gv[band], acc2[band], precision=lax.Precision.HIGHEST, preferred_element_type=F32
        )
    total = jnp.sum(weighted, axis=1, keepdims=True)[0:1] * (1.0 / total_area)
    mine = jnp.where(lax.broadcasted_iota(jnp.int32, (1, 128), 1) == me, total, 0.0)
    for band in range(NLAT):
        zst[band, 1:2, :] = mine

    def copy6(src, dst, band, to):
        return pltpu.make_async_remote_copy(
            src_ref=zst.at[band],
            dst_ref=stats.at[dst],
            send_sem=s6.at[0],
            recv_sem=r6.at[0],
            device_id=to,
            device_id_type=MESH,
        )

    scope("send6")
    for peer in PEERS:
        to, slot = plane(peer)
        copy6(slot, me, lats[peer[0]], to).start()
    for c in near:
        send5((*c, 0))
        send5((*c, 1))
    send5((0, 0, 1))
    field[0, me] = fs[me]
    stats[me] = zst[a]
    scope("wait5")

    whole(st, s1)
    whole(sbuf, s2)
    pltpu.make_async_copy(others, others, s3.at[0]).wait()
    whole(mbuf, s4)
    whole(fs, s5)
    whole(stats, s6)
    whole(field.at[0], r5)
    whole(stats, r6)
    scope(None)


def finish(field, stats, out, zonal, energy, zv, evec, sems):
    big = pltpu.make_async_copy(field, out, sems.at[0])
    big.start()
    gathered = jnp.zeros((1, 128), F32)
    for i in range(CD):
        both = stats[i]
        zv[0, i : i + 1, :] = both[0:1, 0:RD]
        gathered += both[1:2, :]
    evec[...] = gathered[0, 0:CD]
    small = pltpu.make_async_copy(zv, zonal, sems.at[1])
    small.start()
    other = pltpu.make_async_copy(evec, energy, sems.at[2])
    other.start()
    big.wait()
    small.wait()
    other.wait()


def body(state, weights_in, bias_in, weights_out):
    *tabs, total_area = tables()
    hbm = pl.BlockSpec(memory_space=pltpu.HBM)
    vmem = pl.BlockSpec(memory_space=pltpu.VMEM)
    dma = pltpu.SemaphoreType.DMA
    operands = (state, *(jnp.asarray(t) for t in tabs), weights_in, bias_in, weights_out)
    field, stats = pl.pallas_call(
        lambda *refs: kernel(total_area, *refs),
        out_shape=(
            jax.ShapeDtypeStruct((1, CD, RD, ND), BF),
            jax.ShapeDtypeStruct((PLANE, 2, 128), F32),
        ),
        in_specs=[hbm] * 9,
        out_specs=(vmem, vmem),
        scratch_shapes=[
            pltpu.VMEM((CD, RD, ND), BF),
            pltpu.VMEM((LON, 256), BF),
            pltpu.VMEM((256, 2 * LAT), BF),
            pltpu.VMEM((2 * LAT, 256), BF),
            pltpu.VMEM((4, 256, 256), BF),
            pltpu.VMEM((NLAT, 8, RD), F32),
            pltpu.VMEM((2, 256, 256), BF),
            pltpu.VMEM((2, 256, 256), BF),
            pltpu.VMEM((128, 256), F32),
            pltpu.VMEM((PLANE, RD, ND), BF),
            pltpu.VMEM((NLAT, RD, 256), BF),
            pltpu.VMEM((PLANE, 8, 128), BF),
            pltpu.VMEM((PLANE, 8, 128), BF),
            pltpu.VMEM((PLANE * 8, 128), F32),
            pltpu.VMEM((NVAR, CD, 640), BF),
            pltpu.VMEM((PLANE * 8, 128), F32),
            pltpu.VMEM((PLANE, 8, 128), BF),
            pltpu.VMEM((PLANE, 8, 128), BF),
            pltpu.VMEM((NLAT, RD, 256), BF),
            pltpu.VMEM((PLANE, RD, ND), BF),
            pltpu.VMEM((NLAT, RD, 128), F32),
            pltpu.VMEM((NLAT, RD, 128), F32),
            pltpu.VMEM((NLAT, 2, 128), F32),
            dma((9,)),
        ]
        + [dma((1,)), dma((NLAT,))]
        + [dma((1,)), dma((1,))] * 5,
        compiler_params=pltpu.CompilerParams(
            collective_id=0, has_side_effects=True, vmem_limit_bytes=32 * 1024 * 1024
        ),
        name="spectral_layer",
    )(*(pltpu.with_memory_space_constraint(x, pltpu.HBM) for x in operands))
    return pl.pallas_call(
        finish,
        out_shape=(
            jax.ShapeDtypeStruct((1, CD, RD, ND), BF),
            jax.ShapeDtypeStruct((1, CD, RD), F32),
            jax.ShapeDtypeStruct((CD,), F32),
        ),
        in_specs=[vmem, vmem],
        out_specs=(hbm, hbm, hbm),
        scratch_shapes=[
            pltpu.VMEM((1, CD, RD), F32),
            pltpu.VMEM((CD,), F32),
            dma((3,)),
        ],
        compiler_params=pltpu.CompilerParams(vmem_limit_bytes=8 * 1024 * 1024),
        name="finish",
    )(field, stats)


def solution(mesh):
    return jax.shard_map(
        body,
        mesh=mesh,
        in_specs=(P(None, "var", "lat", "lon"), P(), P(), P()),
        out_specs=(P(None, "var", "lat", "lon"), P(None, "var", "lat"), P("var")),
        check_vma=False,
    )
```

```python
import math

import jax
import jax.numpy as jnp
import numpy as np
from jax import lax
from jax.experimental import pallas as pl
from jax.experimental.pallas import tpu as pltpu
from jax.sharding import PartitionSpec as P

LAT = 384
LON = 1024
MLAT = 96
MLON = 96
NVAR = 8
NLAT = 4
NLON = 8
PLANE = NLAT * NLON
CD = 32
RD = LAT // NLAT
ND = LON // NLON
JO = MLAT // PLANE
CH = CD // 2
PIECES = 4
PIECE = CH // PIECES
PITCH = PLANE * 6 + 8
MESH = pl.DeviceIdType.MESH
TAIL_AT = 0.23
TAIL = (
    0.09190782232377631,
    0.08914107185889676,
    0.10610870974692016,
    -0.0007481814870291388,
    0.25362340835459335,
    -0.23501017104744312,
    0.2688627946887361,
    -0.0738853870258165,
)
BF = jnp.bfloat16
F32 = jnp.float32


def ring(d):
    return min(d, 4 - d)


CHIPS = sorted(((i, j) for i in range(4) for j in range(4) if i or j), key=lambda c: -ring(c[0]) - ring(c[1]))
PEERS = [(i, j, c) for i, j in CHIPS for c in range(2)] + [(0, 0, 1)]


def gelu(x):
    size = jnp.abs(x)
    t = 1.0 / (1.0 + TAIL_AT * size)
    poly = TAIL[-1]
    for c in TAIL[-2::-1]:
        poly = poly * t + c
    tail = (size * t) * poly * jnp.exp2((x * x) * (-0.5 / math.log(2.0)))
    return jnp.maximum(x, 0.0) - tail


def tables():
    k = np.arange(MLON)
    n = np.arange(LON)
    angle = 2.0 * np.pi / LON * ((n[:, None] * k[None, :]) % LON)
    scale = 1.0 / math.sqrt(LAT * LON)
    etab = np.zeros((LON, 256), np.float32)
    etab[:, :MLON] = np.cos(angle) * scale
    etab[:, 128 : 128 + MLON] = -np.sin(angle) * scale
    weight = np.where(k == 0, 1.0, 2.0)[:, None] * scale
    full = np.zeros((256, LON), np.float32)
    full[:MLON] = weight * np.cos(angle.T)
    full[128 : 128 + MLON] = -weight * np.sin(angle.T)
    htab = full.reshape(256, 4, 2 * ND).transpose(1, 0, 2)
    r = np.arange(LAT)
    freqs = np.arange(MLAT) - MLAT // 2
    turn = 2.0 * np.pi / LAT * np.mod(freqs[:, None] * r[None, :], LAT)
    cosine, sine = np.cos(turn), np.sin(turn)
    forward = np.zeros((PLANE, 8, 2, LAT), np.float32)
    forward[:, 0:3, 0] = cosine.reshape(PLANE, JO, LAT)
    forward[:, 0:3, 1] = sine.reshape(PLANE, JO, LAT)
    forward[:, 3:6, 0] = -sine.reshape(PLANE, JO, LAT)
    forward[:, 3:6, 1] = cosine.reshape(PLANE, JO, LAT)
    rtab = forward.reshape(PLANE * 8, 2 * LAT).T
    qtab = forward[:, :6].reshape(PLANE * 6, 2, NLAT, RD).transpose(2, 0, 1, 3).reshape(NLAT, PLANE * 6, 2 * RD)
    area = np.cos(np.pi * ((r + 0.5) / LAT - 0.5))
    gtab = np.broadcast_to(area.reshape(NLAT, 1, RD), (NLAT, 8, RD))
    bf = lambda t: np.ascontiguousarray(t).astype(jnp.bfloat16)
    return (
        bf(etab),
        bf(qtab),
        bf(rtab),
        bf(htab),
        np.ascontiguousarray(gtab).astype(np.float32),
        float(LON * area.sum()),
    )


SCOPES = []


def scope(name):
    while SCOPES:
        SCOPES.pop().__exit__(None, None, None)
    if name:
        SCOPES.append(jax.named_scope(name))
        SCOPES[-1].__enter__()


def kernel(
    total_area,
    state,
    etab,
    qtab,
    rtab,
    htab,
    gtab,
    win,
    bias,
    wout,
    field,
    stats,
    st,
    ev,
    qv,
    rv,
    hv,
    gv,
    wiv,
    wov,
    bcol,
    xin,
    ss,
    sa,
    sb,
    ra,
    rb,
    xa,
    xb,
    mf,
    mbuf,
    mrecv,
    lbv,
    fs,
    acc,
    acc2,
    zst,
    load_sem,
    s1,
    r1,
    s2,
    r2,
    s3,
    r3,
    s4,
    r4,
    s5,
    r5,
    s6,
    r6,
):
    v = lax.axis_index("var")
    a = lax.axis_index("lat")
    b = lax.axis_index("lon")
    y, core = lax.div(b, 2), lax.rem(b, 2)

    def slot_of(pa, py, pc):
        return pc * 16 + pa * 4 + py

    me = slot_of(a, y, core)
    lats = [lax.rem(a + i, 4) for i in range(4)]
    ys = [lax.rem(y + i, 4) for i in range(4)]
    cores = [core, 1 - core]

    def plane(peer):
        i, j, c = peer
        pa, py, pc = lats[i], ys[j], cores[c]
        return {"lat": pa, "lon": py * 2 + pc}, slot_of(pa, py, pc)

    loads = [
        pltpu.make_async_copy(src, dst, load_sem.at[i])
        for i, (src, dst) in enumerate(
            [
                (state.at[0, pl.ds(CH * (1 - core), CH)], st.at[1]),
                (state.at[0, pl.ds(CH * core, CH)], st.at[0]),
                (etab.at[pl.ds(b * ND, ND)], ev.at[pl.ds(0, ND)]),
                (etab.at[pl.ds((b + 1 - 2 * core) * ND, ND)], ev.at[pl.ds(ND, ND)]),
                (qtab.at[a], qv),
                (bias, bcol.at[0:2]),
                (win, wiv),
                (wout, wov),
                (rtab, rv),
                (htab, hv),
                (gtab, gv),
            ]
        )
    ]
    loads[0].start()
    loads[1].start()
    scope("greet")
    barrier = pltpu.get_barrier_semaphore()
    for peer in PEERS:
        pl.semaphore_signal(barrier, inc=1, device_id=plane(peer)[0], device_id_type=MESH)
    far = (4, 3, 5, 2, 6, 1, 7)
    vars_ = {d: lax.rem(v + d, NVAR) for d in far}
    for d in far:
        pl.semaphore_signal(barrier, inc=1, device_id={"var": vars_[d]}, device_id_type=MESH)

    for load in loads[2:]:
        load.start()
    mf[...] = jnp.zeros_like(mf)
    zst[...] = jnp.zeros_like(zst)
    acc[...] = jnp.zeros_like(acc)
    acc2[...] = jnp.zeros_like(acc2)
    scope("barrier")
    loads[0].wait()
    pl.semaphore_wait(barrier, PLANE - 1 + NVAR - 1)

    def whole(ref, sem):
        some = ref.at[pl.ds(0, PLANE - 1)]
        pltpu.make_async_copy(some, some, sem.at[0]).wait()

    scope("send1")
    for i in range(PIECES):
        pltpu.make_async_remote_copy(
            src_ref=st.at[1, pl.ds(i * PIECE, PIECE)],
            dst_ref=xin.at[pl.ds(i * PIECE, PIECE)],
            send_sem=s1.at[0],
            recv_sem=r1.at[i],
            device_id={"lon": y * 2 + cores[1]},
            device_id_type=MESH,
        ).start()
    loads[5].wait()
    turned = jnp.transpose(bcol[...])
    for load in loads[1:5]:
        load.wait()

    for i in range(PIECES):
        scope(f"dft{i}")
        some = xin.at[pl.ds(i * PIECE, PIECE)]
        pltpu.make_async_copy(some, some, r1.at[i]).wait()
        chans = slice(i * PIECE, (i + 1) * PIECE)
        both = jnp.concatenate([st[0, chans], xin[chans]], axis=2).reshape(PIECE * RD, 2 * ND)
        lon = jnp.dot(both, ev[...], preferred_element_type=F32).astype(BF)
        for c in range(0, PIECE, 2):
            one, two = lon[c * RD : (c + 1) * RD], lon[(c + 1) * RD : (c + 2) * RD]
            pair = jnp.concatenate(
                [
                    jnp.concatenate([one[:, 0:128], two[:, 0:128]], axis=1),
                    jnp.concatenate([one[:, 128:256], two[:, 128:256]], axis=1),
                ],
                axis=0,
            )
            spec = jnp.dot(qv[...], pair, preferred_element_type=F32)
            at = (i * PIECE + c) * PITCH
            ss[at : at + PLANE * 6, :] = spec[:, 0:128]
            ss[at + PITCH : at + PITCH + PLANE * 6, :] = spec[:, 128:256]

    lane = lax.broadcasted_iota(jnp.int32, (CH, 128), 1)
    low, high = lane < 32, lane >= 96
    second = jnp.logical_and(lane >= 32, lane < 64)

    def pack(slot):
        t = [ss[pl.ds(slot * 6 + i, CH, stride=PITCH), :] for i in range(6)]
        up_r, half_r = pltpu.roll(t[2], 96, 1), pltpu.roll(t[2], 64, 1)
        up_i, half_i = pltpu.roll(t[5], 96, 1), pltpu.roll(t[5], 64, 1)
        p0, p1 = jnp.where(high, up_r, t[0]), jnp.where(high, half_r, t[1])
        p2, p3 = jnp.where(high, up_i, t[3]), jnp.where(high, half_i, t[4])
        p4 = jnp.where(low, half_r, jnp.where(second, up_i, 0.0))
        sa[slot] = jnp.concatenate([p0, p2, p4], axis=1).astype(BF)
        sb[slot] = jnp.concatenate([p1, p3], axis=1).astype(BF)

    def copy2(src_ref, dst_ref, part, peer):
        to, slot = plane(peer)
        return pltpu.make_async_remote_copy(
            src_ref=src_ref.at[slot],
            dst_ref=dst_ref.at[me],
            send_sem=s2.at[part],
            recv_sem=r2.at[part],
            device_id=to,
            device_id_type=MESH,
        )

    scope("pack")
    for peer in PEERS:
        pack(plane(peer)[1])
        copy2(sa, ra, 0, peer).start()
    pack(me)
    for peer in PEERS:
        copy2(sb, rb, 1, peer).start()
    ra[me] = sa[me]
    rb[me] = sb[me]
    bias_r = jnp.broadcast_to(turned[:, 0:1], (256, 128))
    bias_i = jnp.broadcast_to(turned[:, 1:2], (256, 128))

    def whole_at(ref, sem):
        some = ref.at[pl.ds(0, PLANE - 1)]
        pltpu.make_async_copy(some, some, sem).wait()

    def others(ref, sem):
        some = ref.at[pl.ds(0, NVAR - 1)]
        return pltpu.make_async_copy(some, some, sem)

    for part, (got, every) in enumerate(((ra, xa), (rb, xb))):
        scope(f"wait2_{part}")
        whole_at(got, r2.at[part])
        scope(f"sum_{part}")
        for half in range(2):
            total = got[half * CH].astype(F32)
            for i in range(1, CH):
                total += got[half * CH + i].astype(F32)
            every[v, half * CH : (half + 1) * CH] = total.astype(BF)
        for d in far:
            pltpu.make_async_remote_copy(
                src_ref=every.at[v],
                dst_ref=every.at[v],
                send_sem=s3.at[part],
                recv_sem=r3.at[part],
                device_id={"var": vars_[d]},
                device_id_type=MESH,
            ).start()

    scope("wait3")
    for load in loads[6:8]:
        load.wait()
    first = pl.multiple_of(v * CD, CD)
    own = jnp.concatenate([wov[0, pl.ds(first, CD), :], wov[1, pl.ds(first, CD), :]], axis=0)

    def combined(g, half):
        re = g[:half, 0:128] - g[half:, 128:256]
        im = g[half:, 0:128] + g[:half, 128:256]
        if g.shape[1] == 256:
            return re, im
        gr, gi = g[:half, 256:384], g[half:, 256:384]
        which = lax.broadcasted_iota(jnp.int32, (half, 128), 1) < 32
        return re, im, jnp.where(which, gr - pltpu.roll(gi, 96, 1), gr + pltpu.roll(gi, 32, 1))

    def mixed(every, part):
        others(every, r3.at[part]).wait()
        scope(f"mix_{part}")
        g = jnp.dot(wiv[...].reshape(512, 256), every[...].reshape(256, -1), preferred_element_type=F32)
        tiles = combined(g, 256)
        which = lax.broadcasted_iota(jnp.int32, (256, 128), 1) < 32
        biases = (bias_r, bias_i, jnp.where(which, bias_r, bias_i))
        hidden = jnp.concatenate([t + c for t, c in zip(tiles, biases)], axis=1)
        hidden = jnp.maximum(hidden, 0.0).astype(BF)
        return combined(jnp.dot(own, hidden, preferred_element_type=F32), CD)

    re0, im0, last = mixed(xa, 0)
    scope("wait3_1")
    re1, im1 = mixed(xb, 1)
    lane = lax.broadcasted_iota(jnp.int32, (CD, 128), 1)
    sel = [lane < 32, lane < 64]
    t2 = jnp.where(
        sel[0],
        pltpu.roll(re0, 32, 1),
        jnp.where(sel[1], pltpu.roll(re1, 64, 1), pltpu.roll(last, 64, 1)),
    )
    t5 = jnp.where(
        sel[0],
        pltpu.roll(im0, 32, 1),
        jnp.where(sel[1], pltpu.roll(im1, 64, 1), pltpu.roll(last, 32, 1)),
    )
    for i, tile in enumerate([re0, re1, t2, im0, im1, t5]):
        mf[pl.ds(i, PLANE, stride=8), :] = tile
    mbuf[...] = mf[...].reshape(PLANE, 8, 128).astype(BF)

    def copy4(src, dst, to):
        return pltpu.make_async_remote_copy(
            src_ref=mbuf.at[src],
            dst_ref=mrecv.at[dst],
            send_sem=s4.at[0],
            recv_sem=r4.at[0],
            device_id=to,
            device_id_type=MESH,
        )

    scope("send4")
    for peer in PEERS:
        to, slot = plane(peer)
        copy4(slot, me, to).start()
    mrecv[me] = mbuf[me]
    scope("wait4")
    for load in loads[8:]:
        load.wait()
    whole(mrecv, r4)
    scope("back")
    modes = mrecv[...].reshape(PLANE * 8, 128)
    back_r = jnp.dot(rv[0:LAT, :], modes, preferred_element_type=F32)
    back_i = jnp.dot(rv[LAT : 2 * LAT, :], modes, preferred_element_type=F32)
    lbv[...] = jnp.concatenate([back_r, back_i], axis=1).astype(BF).reshape(NLAT, RD, 256)

    def copy5(src, dst, to):
        return pltpu.make_async_remote_copy(
            src_ref=fs.at[src],
            dst_ref=field.at[0, dst],
            send_sem=s5.at[0],
            recv_sem=r5.at[0],
            device_id=to,
            device_id_type=MESH,
        )

    def chip(i, j):
        pa, py = lats[i], ys[j]
        act = gelu(jnp.dot(lbv[pa], hv[py], preferred_element_type=F32))
        fs[slot_of(pa, py, 0)] = act[:, 0:128].astype(BF)
        fs[slot_of(pa, py, 1)] = act[:, 128:256].astype(BF)
        acc[pa] += act[:, 0:128] + act[:, 128:256]
        square = act * act
        acc2[pa] += square[:, 0:128] + square[:, 128:256]

    def send5(peer):
        to, slot = plane(peer)
        copy5(slot, me, to).start()

    scope("gelu")
    near = [c for c in CHIPS if ring(c[0]) + ring(c[1]) <= 2]
    for c in CHIPS:
        chip(*c)
        if c not in near:
            send5((*c, 0))
            send5((*c, 1))
    chip(0, 0)
    scope("stats")
    ones = jnp.ones((8, 128), F32)
    weighted = jnp.zeros((8, 128), F32)
    for band in range(NLAT):
        rowsum = lax.dot_general(
            ones,
            acc[band],
            (((1,), (1,)), ((), ())),
            precision=lax.Precision.HIGHEST,
            preferred_element_type=F32,
        )
        zst[band, 0:1, 0:RD] = rowsum[0:1] * (1.0 / LON)
        weighted += jnp.dot(
            gv[band], acc2[band], precision=lax.Precision.HIGHEST, preferred_element_type=F32
        )
    total = jnp.sum(weighted, axis=1, keepdims=True)[0:1] * (1.0 / total_area)
    mine = jnp.where(lax.broadcasted_iota(jnp.int32, (1, 128), 1) == me, total, 0.0)
    for band in range(NLAT):
        zst[band, 1:2, :] = mine

    def copy6(src, dst, band, to):
        return pltpu.make_async_remote_copy(
            src_ref=zst.at[band],
            dst_ref=stats.at[dst],
            send_sem=s6.at[0],
            recv_sem=r6.at[0],
            device_id=to,
            device_id_type=MESH,
        )

    scope("send6")
    for peer in PEERS:
        to, slot = plane(peer)
        copy6(slot, me, lats[peer[0]], to).start()
    for c in near:
        send5((*c, 0))
        send5((*c, 1))
    send5((0, 0, 1))
    field[0, me] = fs[me]
    stats[me] = zst[a]
    scope("wait5")

    pltpu.make_async_copy(xin, xin, s1.at[0]).wait()
    whole_at(sa, s2.at[0])
    whole_at(sb, s2.at[1])
    others(xa, s3.at[0]).wait()
    others(xb, s3.at[1]).wait()
    whole(mbuf, s4)
    whole(fs, s5)
    whole(stats, s6)
    whole(field.at[0], r5)
    whole(stats, r6)
    scope(None)


def finish(field, stats, out, zonal, energy, zv, evec, sems):
    big = pltpu.make_async_copy(field, out, sems.at[0])
    big.start()
    gathered = jnp.zeros((1, 128), F32)
    for i in range(CD):
        both = stats[i]
        zv[0, i : i + 1, :] = both[0:1, 0:RD]
        gathered += both[1:2, :]
    evec[...] = gathered[0, 0:CD]
    small = pltpu.make_async_copy(zv, zonal, sems.at[1])
    small.start()
    other = pltpu.make_async_copy(evec, energy, sems.at[2])
    other.start()
    big.wait()
    small.wait()
    other.wait()


def body(state, weights_in, bias_in, weights_out):
    *tabs, total_area = tables()
    hbm = pl.BlockSpec(memory_space=pltpu.HBM)
    vmem = pl.BlockSpec(memory_space=pltpu.VMEM)
    dma = pltpu.SemaphoreType.DMA
    operands = (state, *(jnp.asarray(t) for t in tabs), weights_in, bias_in, weights_out)
    field, stats = pl.pallas_call(
        lambda *refs: kernel(total_area, *refs),
        out_shape=(
            jax.ShapeDtypeStruct((1, CD, RD, ND), BF),
            jax.ShapeDtypeStruct((PLANE, 2, 128), F32),
        ),
        in_specs=[hbm] * 9,
        out_specs=(vmem, vmem),
        scratch_shapes=[
            pltpu.VMEM((2, CH, RD, ND), BF),
            pltpu.VMEM((2 * ND, 256), BF),
            pltpu.VMEM((PLANE * 6, 2 * RD), BF),
            pltpu.VMEM((2 * LAT, 256), BF),
            pltpu.VMEM((4, 256, 256), BF),
            pltpu.VMEM((NLAT, 8, RD), F32),
            pltpu.VMEM((2, 256, 256), BF),
            pltpu.VMEM((2, 256, 256), BF),
            pltpu.VMEM((128, 256), F32),
            pltpu.VMEM((CH, RD, ND), BF),
            pltpu.VMEM((CH * PITCH, 128), F32),
            pltpu.VMEM((PLANE, CH, 384), BF),
            pltpu.VMEM((PLANE, CH, 256), BF),
            pltpu.VMEM((PLANE, CH, 384), BF),
            pltpu.VMEM((PLANE, CH, 256), BF),
            pltpu.VMEM((NVAR, CD, 384), BF),
            pltpu.VMEM((NVAR, CD, 256), BF),
            pltpu.VMEM((PLANE * 8, 128), F32),
            pltpu.VMEM((PLANE, 8, 128), BF),
            pltpu.VMEM((PLANE, 8, 128), BF),
            pltpu.VMEM((NLAT, RD, 256), BF),
            pltpu.VMEM((PLANE, RD, ND), BF),
            pltpu.VMEM((NLAT, RD, 128), F32),
            pltpu.VMEM((NLAT, RD, 128), F32),
            pltpu.VMEM((NLAT, 2, 128), F32),
            dma((11,)),
        ]
        + [dma((1,)), dma((PIECES,)), dma((2,)), dma((2,)), dma((2,)), dma((2,))]
        + [dma((1,)), dma((1,))] * 3,
        compiler_params=pltpu.CompilerParams(
            collective_id=0, has_side_effects=True, vmem_limit_bytes=32 * 1024 * 1024
        ),
        name="spectral_layer",
    )(*(pltpu.with_memory_space_constraint(x, pltpu.HBM) for x in operands))
    return pl.pallas_call(
        finish,
        out_shape=(
            jax.ShapeDtypeStruct((1, CD, RD, ND), BF),
            jax.ShapeDtypeStruct((1, CD, RD), F32),
            jax.ShapeDtypeStruct((CD,), F32),
        ),
        in_specs=[vmem, vmem],
        out_specs=(hbm, hbm, hbm),
        scratch_shapes=[
            pltpu.VMEM((1, CD, RD), F32),
            pltpu.VMEM((CD,), F32),
            dma((3,)),
        ],
        compiler_params=pltpu.CompilerParams(vmem_limit_bytes=8 * 1024 * 1024),
        name="finish",
    )(field, stats)


def solution(mesh):
    return jax.shard_map(
        body,
        mesh=mesh,
        in_specs=(P(None, "var", "lat", "lon"), P(), P(), P()),
        out_specs=(P(None, "var", "lat", "lon"), P(None, "var", "lat"), P("var")),
        check_vma=False,
    )
```

```python
import math

import jax
import jax.numpy as jnp
import numpy as np
from jax import lax
from jax.experimental import pallas as pl
from jax.experimental.pallas import tpu as pltpu
from jax.sharding import PartitionSpec as P

LAT = 384
LON = 1024
MLAT = 96
MLON = 96
NVAR = 8
NLAT = 4
NLON = 8
PLANE = NLAT * NLON
CD = 32
RD = LAT // NLAT
ND = LON // NLON
JO = MLAT // PLANE
CH = CD // 2
PIECES = 2
PIECE = CH // PIECES
PITCH = PLANE * 6 + 8
MESH = pl.DeviceIdType.MESH
TAIL_AT = 0.23
TAIL = (
    0.09190782232377631,
    0.08914107185889676,
    0.10610870974692016,
    -0.0007481814870291388,
    0.25362340835459335,
    -0.23501017104744312,
    0.2688627946887361,
    -0.0738853870258165,
)
BF = jnp.bfloat16
F32 = jnp.float32


def ring(d):
    return min(d, 4 - d)


CHIPS = sorted(((i, j) for i in range(4) for j in range(4) if i or j), key=lambda c: -ring(c[0]) - ring(c[1]))
PEERS = [(i, j, c) for i, j in CHIPS for c in range(2)] + [(0, 0, 1)]


def gelu(x):
    size = jnp.abs(x)
    t = 1.0 / (1.0 + TAIL_AT * size)
    poly = TAIL[-1]
    for c in TAIL[-2::-1]:
        poly = poly * t + c
    tail = (size * t) * poly * jnp.exp2((x * x) * (-0.5 / math.log(2.0)))
    return jnp.maximum(x, 0.0) - tail


def tables():
    k = np.arange(MLON)
    n = np.arange(LON)
    angle = 2.0 * np.pi / LON * ((n[:, None] * k[None, :]) % LON)
    scale = 1.0 / math.sqrt(LAT * LON)
    etab = np.zeros((LON, 256), np.float32)
    etab[:, :MLON] = np.cos(angle) * scale
    etab[:, 128 : 128 + MLON] = -np.sin(angle) * scale
    weight = np.where(k == 0, 1.0, 2.0)[:, None] * scale
    full = np.zeros((256, LON), np.float32)
    full[:MLON] = weight * np.cos(angle.T)
    full[128 : 128 + MLON] = -weight * np.sin(angle.T)
    htab = full.reshape(256, 4, 2 * ND).transpose(1, 0, 2)
    r = np.arange(LAT)
    freqs = np.arange(MLAT) - MLAT // 2
    turn = 2.0 * np.pi / LAT * np.mod(freqs[:, None] * r[None, :], LAT)
    cosine, sine = np.cos(turn), np.sin(turn)
    forward = np.zeros((PLANE, 8, 2, LAT), np.float32)
    forward[:, 0:3, 0] = cosine.reshape(PLANE, JO, LAT)
    forward[:, 0:3, 1] = sine.reshape(PLANE, JO, LAT)
    forward[:, 3:6, 0] = -sine.reshape(PLANE, JO, LAT)
    forward[:, 3:6, 1] = cosine.reshape(PLANE, JO, LAT)
    rtab = forward.reshape(PLANE * 8, 2 * LAT).T
    qtab = forward[:, :6].reshape(PLANE * 6, 2, NLAT, RD).transpose(2, 0, 1, 3).reshape(NLAT, PLANE * 6, 2 * RD)
    area = np.cos(np.pi * ((r + 0.5) / LAT - 0.5))
    gtab = np.broadcast_to(area.reshape(NLAT, 1, RD), (NLAT, 8, RD))
    bf = lambda t: np.ascontiguousarray(t).astype(jnp.bfloat16)
    return (
        bf(etab),
        bf(qtab),
        bf(rtab),
        bf(htab),
        np.ascontiguousarray(gtab).astype(np.float32),
        float(LON * area.sum()),
    )


SCOPES = []


def scope(name):
    while SCOPES:
        SCOPES.pop().__exit__(None, None, None)
    if name:
        SCOPES.append(jax.named_scope(name))
        SCOPES[-1].__enter__()


def kernel(
    total_area,
    state,
    etab,
    qtab,
    rtab,
    htab,
    gtab,
    win,
    bias,
    wout,
    field,
    stats,
    st,
    ev,
    qv,
    rv,
    hv,
    gv,
    wiv,
    wov,
    bcol,
    xin,
    ss,
    sa,
    sb,
    sc,
    ra,
    rb,
    rc,
    xa,
    xb,
    xc,
    mf,
    mbuf,
    mrecv,
    lbv,
    fs,
    acc,
    acc2,
    zst,
    load_sem,
    s1,
    r1,
    s2,
    r2,
    s3,
    r3,
    s4,
    r4,
    s5,
    r5,
    s6,
    r6,
):
    v = lax.axis_index("var")
    a = lax.axis_index("lat")
    b = lax.axis_index("lon")
    y, core = lax.div(b, 2), lax.rem(b, 2)

    def slot_of(pa, py, pc):
        return pc * 16 + pa * 4 + py

    me = slot_of(a, y, core)
    lats = [lax.rem(a + i, 4) for i in range(4)]
    ys = [lax.rem(y + i, 4) for i in range(4)]
    cores = [core, 1 - core]

    def plane(peer):
        i, j, c = peer
        pa, py, pc = lats[i], ys[j], cores[c]
        return {"lat": pa, "lon": py * 2 + pc}, slot_of(pa, py, pc)

    loads = [
        pltpu.make_async_copy(src, dst, load_sem.at[i])
        for i, (src, dst) in enumerate(
            [
                (state.at[0, pl.ds(CH * (1 - core), CH)], st.at[1]),
                (state.at[0, pl.ds(CH * core, CH)], st.at[0]),
                (etab.at[pl.ds(b * ND, ND)], ev.at[pl.ds(0, ND)]),
                (etab.at[pl.ds((b + 1 - 2 * core) * ND, ND)], ev.at[pl.ds(ND, ND)]),
                (qtab.at[a], qv),
                (bias, bcol.at[0:2]),
                (win, wiv),
                (wout, wov),
                (rtab, rv),
                (htab, hv),
                (gtab, gv),
            ]
        )
    ]
    loads[0].start()
    loads[1].start()
    scope("greet")
    barrier = pltpu.get_barrier_semaphore()
    for peer in PEERS:
        pl.semaphore_signal(barrier, inc=1, device_id=plane(peer)[0], device_id_type=MESH)
    far = (4, 3, 5, 2, 6, 1, 7)
    vars_ = {d: lax.rem(v + d, NVAR) for d in far}
    for d in far:
        pl.semaphore_signal(barrier, inc=1, device_id={"var": vars_[d]}, device_id_type=MESH)

    for load in loads[2:]:
        load.start()
    mf[...] = jnp.zeros_like(mf)
    zst[...] = jnp.zeros_like(zst)
    acc[...] = jnp.zeros_like(acc)
    acc2[...] = jnp.zeros_like(acc2)
    scope("barrier")
    loads[0].wait()
    scope("barrier2")
    pl.semaphore_wait(barrier, PLANE - 1 + NVAR - 1)

    def whole(ref, sem):
        some = ref.at[pl.ds(0, PLANE - 1)]
        pltpu.make_async_copy(some, some, sem.at[0]).wait()

    scope("send1")
    for i in range(PIECES):
        pltpu.make_async_remote_copy(
            src_ref=st.at[1, pl.ds(i * PIECE, PIECE)],
            dst_ref=xin.at[pl.ds(i * PIECE, PIECE)],
            send_sem=s1.at[0],
            recv_sem=r1.at[i],
            device_id={"lon": y * 2 + cores[1]},
            device_id_type=MESH,
        ).start()
    loads[5].wait()
    turned = jnp.transpose(bcol[...])
    for load in loads[1:5]:
        load.wait()

    for i in range(PIECES):
        scope(f"dft{i}")
        some = xin.at[pl.ds(i * PIECE, PIECE)]
        pltpu.make_async_copy(some, some, r1.at[i]).wait()
        chans = slice(i * PIECE, (i + 1) * PIECE)
        both = jnp.concatenate([st[0, chans], xin[chans]], axis=2).reshape(PIECE * RD, 2 * ND)
        lon = jnp.dot(both, ev[...], preferred_element_type=F32).astype(BF)
        for c in range(0, PIECE, 2):
            one, two = lon[c * RD : (c + 1) * RD], lon[(c + 1) * RD : (c + 2) * RD]
            pair = jnp.concatenate(
                [
                    jnp.concatenate([one[:, 0:128], two[:, 0:128]], axis=1),
                    jnp.concatenate([one[:, 128:256], two[:, 128:256]], axis=1),
                ],
                axis=0,
            )
            spec = jnp.dot(qv[...], pair, preferred_element_type=F32)
            at = (i * PIECE + c) * PITCH
            ss[at : at + PLANE * 6, :] = spec[:, 0:128]
            ss[at + PITCH : at + PITCH + PLANE * 6, :] = spec[:, 128:256]

    lane = lax.broadcasted_iota(jnp.int32, (CH, 128), 1)
    low, high = lane < 32, lane >= 96
    second = jnp.logical_and(lane >= 32, lane < 64)

    def pack(slot):
        t = [ss[pl.ds(slot * 6 + i, CH, stride=PITCH), :] for i in range(6)]
        up_r, half_r = pltpu.roll(t[2], 96, 1), pltpu.roll(t[2], 64, 1)
        up_i, half_i = pltpu.roll(t[5], 96, 1), pltpu.roll(t[5], 64, 1)
        p0, p1 = jnp.where(high, up_r, t[0]), jnp.where(high, half_r, t[1])
        p2, p3 = jnp.where(high, up_i, t[3]), jnp.where(high, half_i, t[4])
        p4 = jnp.where(low, half_r, jnp.where(second, up_i, 0.0))
        sa[slot] = jnp.concatenate([p0, p2], axis=1).astype(BF)
        sb[slot] = jnp.concatenate([p1, p3], axis=1).astype(BF)
        sc[slot] = (p4[0:8] + pltpu.roll(p4[8:16], 64, 1)).astype(BF)

    def copy2(src_ref, dst_ref, part, peer):
        to, slot = plane(peer)
        return pltpu.make_async_remote_copy(
            src_ref=src_ref.at[slot],
            dst_ref=dst_ref.at[me],
            send_sem=s2.at[part],
            recv_sem=r2.at[part],
            device_id=to,
            device_id_type=MESH,
        )

    scope("pack")
    for i in range(0, len(PEERS), 8):
        for peer in PEERS[i : i + 8]:
            pack(plane(peer)[1])
        for peer in PEERS[i : i + 8]:
            copy2(sa, ra, 0, peer).start()
    for peer in PEERS:
        copy2(sb, rb, 1, peer).start()
    for peer in PEERS:
        copy2(sc, rc, 2, peer).start()
    pack(me)
    ra[me] = sa[me]
    rb[me] = sb[me]
    rc[me] = sc[me]
    bias_r = jnp.broadcast_to(turned[:, 0:1], (256, 128))
    bias_i = jnp.broadcast_to(turned[:, 1:2], (256, 128))

    def whole_at(ref, sem):
        some = ref.at[pl.ds(0, PLANE - 1)]
        pltpu.make_async_copy(some, some, sem).wait()

    def others(ref, sem):
        some = ref.at[pl.ds(0, NVAR - 1)]
        return pltpu.make_async_copy(some, some, sem)

    for part, (got, every) in enumerate(((ra, xa), (rb, xb), (rc, xc))):
        scope(f"wait2_{part}")
        whole_at(got, r2.at[part])
        scope(f"sum_{part}")
        for half in range(2):
            total = got[half * CH].astype(F32)
            for i in range(1, CH):
                total += got[half * CH + i].astype(F32)
            rows = got.shape[1]
            every[v, half * rows : (half + 1) * rows] = total.astype(BF)
        for d in far:
            pltpu.make_async_remote_copy(
                src_ref=every.at[v],
                dst_ref=every.at[v],
                send_sem=s3.at[part],
                recv_sem=r3.at[part],
                device_id={"var": vars_[d]},
                device_id_type=MESH,
            ).start()

    scope("wait3")
    for load in loads[6:8]:
        load.wait()
    first = pl.multiple_of(v * CD, CD)
    own = jnp.concatenate([wov[0, pl.ds(first, CD), :], wov[1, pl.ds(first, CD), :]], axis=0)

    def combined(g, half):
        if g.shape[1] == 256:
            return g[:half, 0:128] - g[half:, 128:256], g[half:, 0:128] + g[:half, 128:256]
        which = lax.broadcasted_iota(jnp.int32, (half, 128), 1) < 32
        gr, gi = g[:half], g[half:]
        return (jnp.where(which, gr - pltpu.roll(gi, 96, 1), gr + pltpu.roll(gi, 32, 1)),)

    def mixed(every, part):
        others(every, r3.at[part]).wait()
        scope(f"mix_{part}")
        if every is xc:
            folded = xc[...].astype(F32).reshape(2 * NVAR, 8, 128)
            beside = pltpu.roll(folded, 64, 2)
            rows = jnp.stack([folded, beside], axis=1).reshape(256, 128).astype(BF)
        else:
            rows = every[...].reshape(256, -1)
        g = jnp.dot(wiv[...].reshape(512, 256), rows, preferred_element_type=F32)
        tiles = combined(g, 256)
        which = lax.broadcasted_iota(jnp.int32, (256, 128), 1) < 32
        biases = (bias_r, bias_i) if len(tiles) == 2 else (jnp.where(which, bias_r, bias_i),)
        hidden = jnp.concatenate([t + c for t, c in zip(tiles, biases)], axis=1)
        hidden = jnp.maximum(hidden, 0.0).astype(BF)
        return combined(jnp.dot(own, hidden, preferred_element_type=F32), CD)

    lane = lax.broadcasted_iota(jnp.int32, (CD, 128), 1)

    def put(i, tile):
        mf[pl.ds(i, PLANE, stride=8), :] = tile

    re0, im0 = mixed(xa, 0)
    put(0, re0)
    put(3, im0)
    scope("wait3_1")
    re1, im1 = mixed(xb, 1)
    put(1, re1)
    put(4, im1)
    kept_r = jnp.where(lane < 32, pltpu.roll(re0, 32, 1), pltpu.roll(re1, 64, 1))
    kept_i = jnp.where(lane < 32, pltpu.roll(im0, 32, 1), pltpu.roll(im1, 64, 1))
    scope("wait3_2")
    (last,) = mixed(xc, 2)
    put(2, jnp.where(lane < 64, kept_r, pltpu.roll(last, 64, 1)))
    put(5, jnp.where(lane < 64, kept_i, pltpu.roll(last, 32, 1)))
    mbuf[...] = mf[...].reshape(PLANE, 8, 128).astype(BF)

    def copy4(src, dst, to):
        return pltpu.make_async_remote_copy(
            src_ref=mbuf.at[src],
            dst_ref=mrecv.at[dst],
            send_sem=s4.at[0],
            recv_sem=r4.at[0],
            device_id=to,
            device_id_type=MESH,
        )

    scope("send4")
    for peer in PEERS:
        to, slot = plane(peer)
        copy4(slot, me, to).start()
    mrecv[me] = mbuf[me]
    scope("wait4")
    for load in loads[8:]:
        load.wait()
    whole(mrecv, r4)
    scope("back")
    modes = mrecv[...].reshape(PLANE * 8, 128)
    back_r = jnp.dot(rv[0:LAT, :], modes, preferred_element_type=F32)
    back_i = jnp.dot(rv[LAT : 2 * LAT, :], modes, preferred_element_type=F32)
    lbv[...] = jnp.concatenate([back_r, back_i], axis=1).astype(BF).reshape(NLAT, RD, 256)

    def copy5(src, dst, to):
        return pltpu.make_async_remote_copy(
            src_ref=fs.at[src],
            dst_ref=field.at[0, dst],
            send_sem=s5.at[0],
            recv_sem=r5.at[0],
            device_id=to,
            device_id_type=MESH,
        )

    def chip(i, j):
        pa, py = lats[i], ys[j]
        act = gelu(jnp.dot(lbv[pa], hv[py], preferred_element_type=F32))
        fs[slot_of(pa, py, 0)] = act[:, 0:128].astype(BF)
        fs[slot_of(pa, py, 1)] = act[:, 128:256].astype(BF)
        acc[pa] += act[:, 0:128] + act[:, 128:256]
        square = act * act
        acc2[pa] += square[:, 0:128] + square[:, 128:256]

    def send5(peer):
        to, slot = plane(peer)
        copy5(slot, me, to).start()

    scope("gelu")
    near = [c for c in CHIPS if ring(c[0]) + ring(c[1]) <= 1]
    for c in CHIPS:
        chip(*c)
        if c not in near:
            send5((*c, 0))
            send5((*c, 1))
    chip(0, 0)
    scope("stats")
    ones = jnp.ones((8, 128), F32)
    weighted = jnp.zeros((8, 128), F32)
    for band in range(NLAT):
        rowsum = lax.dot_general(
            ones,
            acc[band],
            (((1,), (1,)), ((), ())),
            precision=lax.Precision.HIGHEST,
            preferred_element_type=F32,
        )
        zst[band, 0:1, 0:RD] = rowsum[0:1] * (1.0 / LON)
        weighted += jnp.dot(
            gv[band], acc2[band], precision=lax.Precision.HIGHEST, preferred_element_type=F32
        )
    total = jnp.sum(weighted, axis=1, keepdims=True)[0:1] * (1.0 / total_area)
    mine = jnp.where(lax.broadcasted_iota(jnp.int32, (1, 128), 1) == me, total, 0.0)
    for band in range(NLAT):
        zst[band, 1:2, :] = mine

    def copy6(src, dst, band, to):
        return pltpu.make_async_remote_copy(
            src_ref=zst.at[band],
            dst_ref=stats.at[dst],
            send_sem=s6.at[0],
            recv_sem=r6.at[0],
            device_id=to,
            device_id_type=MESH,
        )

    scope("send6")
    for peer in PEERS:
        to, slot = plane(peer)
        copy6(slot, me, lats[peer[0]], to).start()
    for c in near:
        send5((*c, 0))
        send5((*c, 1))
    send5((0, 0, 1))
    field[0, me] = fs[me]
    stats[me] = zst[a]
    scope("wait5")

    pltpu.make_async_copy(xin, xin, s1.at[0]).wait()
    whole_at(sa, s2.at[0])
    whole_at(sb, s2.at[1])
    whole_at(sc, s2.at[2])
    others(xa, s3.at[0]).wait()
    others(xb, s3.at[1]).wait()
    others(xc, s3.at[2]).wait()
    whole(mbuf, s4)
    whole(fs, s5)
    whole(stats, s6)
    whole(field.at[0], r5)
    whole(stats, r6)
    scope(None)


def finish(field, stats, out, zonal, energy, zv, evec, sems):
    big = pltpu.make_async_copy(field, out, sems.at[0])
    big.start()
    gathered = jnp.zeros((1, 128), F32)
    for i in range(CD):
        both = stats[i]
        zv[0, i : i + 1, :] = both[0:1, 0:RD]
        gathered += both[1:2, :]
    evec[...] = gathered[0, 0:CD]
    small = pltpu.make_async_copy(zv, zonal, sems.at[1])
    small.start()
    other = pltpu.make_async_copy(evec, energy, sems.at[2])
    other.start()
    big.wait()
    small.wait()
    other.wait()


def body(state, weights_in, bias_in, weights_out):
    *tabs, total_area = tables()
    hbm = pl.BlockSpec(memory_space=pltpu.HBM)
    vmem = pl.BlockSpec(memory_space=pltpu.VMEM)
    dma = pltpu.SemaphoreType.DMA
    operands = (state, *(jnp.asarray(t) for t in tabs), weights_in, bias_in, weights_out)
    field, stats = pl.pallas_call(
        lambda *refs: kernel(total_area, *refs),
        out_shape=(
            jax.ShapeDtypeStruct((1, CD, RD, ND), BF),
            jax.ShapeDtypeStruct((PLANE, 2, 128), F32),
        ),
        in_specs=[hbm] * 9,
        out_specs=(vmem, vmem),
        scratch_shapes=[
            pltpu.VMEM((2, CH, RD, ND), BF),
            pltpu.VMEM((2 * ND, 256), BF),
            pltpu.VMEM((PLANE * 6, 2 * RD), BF),
            pltpu.VMEM((2 * LAT, 256), BF),
            pltpu.VMEM((4, 256, 256), BF),
            pltpu.VMEM((NLAT, 8, RD), F32),
            pltpu.VMEM((2, 256, 256), BF),
            pltpu.VMEM((2, 256, 256), BF),
            pltpu.VMEM((128, 256), F32),
            pltpu.VMEM((CH, RD, ND), BF),
            pltpu.VMEM((CH * PITCH, 128), F32),
            pltpu.VMEM((PLANE, CH, 256), BF),
            pltpu.VMEM((PLANE, CH, 256), BF),
            pltpu.VMEM((PLANE, 8, 128), BF),
            pltpu.VMEM((PLANE, CH, 256), BF),
            pltpu.VMEM((PLANE, CH, 256), BF),
            pltpu.VMEM((PLANE, 8, 128), BF),
            pltpu.VMEM((NVAR, CD, 256), BF),
            pltpu.VMEM((NVAR, CD, 256), BF),
            pltpu.VMEM((NVAR, CH, 128), BF),
            pltpu.VMEM((PLANE * 8, 128), F32),
            pltpu.VMEM((PLANE, 8, 128), BF),
            pltpu.VMEM((PLANE, 8, 128), BF),
            pltpu.VMEM((NLAT, RD, 256), BF),
            pltpu.VMEM((PLANE, RD, ND), BF),
            pltpu.VMEM((NLAT, RD, 128), F32),
            pltpu.VMEM((NLAT, RD, 128), F32),
            pltpu.VMEM((NLAT, 2, 128), F32),
            dma((11,)),
        ]
        + [dma((1,)), dma((PIECES,)), dma((3,)), dma((3,)), dma((3,)), dma((3,))]
        + [dma((1,)), dma((1,))] * 3,
        compiler_params=pltpu.CompilerParams(
            collective_id=0, has_side_effects=True, vmem_limit_bytes=32 * 1024 * 1024
        ),
        name="spectral_layer",
    )(*(pltpu.with_memory_space_constraint(x, pltpu.HBM) for x in operands))
    return pl.pallas_call(
        finish,
        out_shape=(
            jax.ShapeDtypeStruct((1, CD, RD, ND), BF),
            jax.ShapeDtypeStruct((1, CD, RD), F32),
            jax.ShapeDtypeStruct((CD,), F32),
        ),
        in_specs=[vmem, vmem],
        out_specs=(hbm, hbm, hbm),
        scratch_shapes=[
            pltpu.VMEM((1, CD, RD), F32),
            pltpu.VMEM((CD,), F32),
            dma((3,)),
        ],
        compiler_params=pltpu.CompilerParams(vmem_limit_bytes=8 * 1024 * 1024),
        name="finish",
    )(field, stats)


def solution(mesh):
    return jax.shard_map(
        body,
        mesh=mesh,
        in_specs=(P(None, "var", "lat", "lon"), P(), P(), P()),
        out_specs=(P(None, "var", "lat", "lon"), P(None, "var", "lat"), P("var")),
        check_vma=False,
    )
```

```python
import math

import jax
import jax.numpy as jnp
import numpy as np
from jax import lax
from jax.experimental import pallas as pl
from jax.experimental.pallas import tpu as pltpu
from jax.sharding import PartitionSpec as P

LAT = 384
LON = 1024
MLAT = 96
MLON = 96
NVAR = 8
NLAT = 4
NLON = 8
PLANE = NLAT * NLON
CD = 32
RD = LAT // NLAT
ND = LON // NLON
JO = MLAT // PLANE
CH = CD // 2
PIECES = 2
PIECE = CH // PIECES
PITCH = PLANE * 6 + 8
MESH = pl.DeviceIdType.MESH
TAIL_AT = 0.23
TAIL = (
    0.09190782232377631,
    0.08914107185889676,
    0.10610870974692016,
    -0.0007481814870291388,
    0.25362340835459335,
    -0.23501017104744312,
    0.2688627946887361,
    -0.0738853870258165,
)
BF = jnp.bfloat16
F32 = jnp.float32


def ring(d):
    return min(d, 4 - d)


CHIPS = sorted(((i, j) for i in range(4) for j in range(4) if i or j), key=lambda c: -ring(c[0]) - ring(c[1]))
PEERS = [(i, j, c) for i, j in CHIPS for c in range(2)] + [(0, 0, 1)]


def gelu(x):
    size = jnp.abs(x)
    t = 1.0 / (1.0 + TAIL_AT * size)
    poly = TAIL[-1]
    for c in TAIL[-2::-1]:
        poly = poly * t + c
    tail = (size * t) * poly * jnp.exp2((x * x) * (-0.5 / math.log(2.0)))
    return jnp.maximum(x, 0.0) - tail


def tables():
    k = np.arange(MLON)
    n = np.arange(LON)
    angle = 2.0 * np.pi / LON * ((n[:, None] * k[None, :]) % LON)
    scale = 1.0 / math.sqrt(LAT * LON)
    etab = np.zeros((LON, 256), np.float32)
    etab[:, :MLON] = np.cos(angle) * scale
    etab[:, 128 : 128 + MLON] = -np.sin(angle) * scale
    weight = np.where(k == 0, 1.0, 2.0)[:, None] * scale
    full = np.zeros((256, LON), np.float32)
    full[:MLON] = weight * np.cos(angle.T)
    full[128 : 128 + MLON] = -weight * np.sin(angle.T)
    htab = full.reshape(256, NLON, ND).transpose(1, 0, 2)
    r = np.arange(LAT)
    freqs = np.arange(MLAT) - MLAT // 2
    turn = 2.0 * np.pi / LAT * np.mod(freqs[:, None] * r[None, :], LAT)
    cosine, sine = np.cos(turn), np.sin(turn)
    forward = np.zeros((PLANE, 6, 2, LAT), np.float32)
    forward[:, 0:3, 0] = cosine.reshape(PLANE, JO, LAT)
    forward[:, 0:3, 1] = sine.reshape(PLANE, JO, LAT)
    forward[:, 3:6, 0] = -sine.reshape(PLANE, JO, LAT)
    forward[:, 3:6, 1] = cosine.reshape(PLANE, JO, LAT)
    qtab = forward.reshape(PLANE * 6, 2, NLAT, RD).transpose(2, 0, 1, 3).reshape(NLAT, PLANE * 6, 2 * RD)
    rtab = qtab.transpose(0, 2, 1)
    area = np.cos(np.pi * ((r + 0.5) / LAT - 0.5))
    gtab = np.broadcast_to(area.reshape(NLAT, RD, 1), (NLAT, RD, 128))
    bf = lambda t: np.ascontiguousarray(t).astype(jnp.bfloat16)
    return (
        bf(etab),
        bf(qtab),
        bf(rtab),
        bf(htab),
        np.ascontiguousarray(gtab).astype(np.float32),
        float(LON * area.sum()),
    )


SCOPES = []


def scope(name):
    while SCOPES:
        SCOPES.pop().__exit__(None, None, None)
    if name:
        SCOPES.append(jax.named_scope(name))
        SCOPES[-1].__enter__()


def kernel(
    state,
    etab,
    qtab,
    rtab,
    htab,
    gtab,
    win,
    bias,
    wout,
    field,
    zrec,
    erec,
    st,
    ev,
    qv,
    rv,
    hv,
    gv,
    wiv,
    wov,
    bcol,
    xin,
    ss,
    sa,
    sb,
    sc,
    ra,
    rb,
    rc,
    xa,
    xb,
    xc,
    ma,
    mb,
    mc,
    ba,
    bb,
    bc,
    fs,
    zacc,
    eacc,
    zmsg,
    emsg,
    load_sem,
    s1,
    r1,
    s2,
    r2,
    s3,
    r3,
    s4,
    r4,
    s5,
    r5,
    s6,
    r6,
    s7,
    r7,
):
    v = lax.axis_index("var")
    a = lax.axis_index("lat")
    b = lax.axis_index("lon")
    y, core = lax.div(b, 2), lax.rem(b, 2)

    def slot_of(pa, py, pc):
        return pc * 16 + pa * 4 + py

    me = slot_of(a, y, core)
    lats = [lax.rem(a + i, 4) for i in range(4)]
    ys = [lax.rem(y + i, 4) for i in range(4)]
    cores = [core, 1 - core]

    def plane(peer):
        i, j, c = peer
        pa, py, pc = lats[i], ys[j], cores[c]
        return {"lat": pa, "lon": py * 2 + pc}, slot_of(pa, py, pc)

    loads = [
        pltpu.make_async_copy(src, dst, load_sem.at[i])
        for i, (src, dst) in enumerate(
            [
                (state.at[0, pl.ds(CH * (1 - core), CH)], st.at[1]),
                (state.at[0, pl.ds(CH * core, CH)], st.at[0]),
                (etab.at[pl.ds(b * ND, ND)], ev.at[pl.ds(0, ND)]),
                (etab.at[pl.ds((b + 1 - 2 * core) * ND, ND)], ev.at[pl.ds(ND, ND)]),
                (qtab.at[a], qv),
                (bias, bcol.at[0:2]),
                (win, wiv),
                (wout, wov),
                (rtab.at[a], rv),
                (htab.at[b], hv.at[:, pl.ds(0, ND)]),
                (htab.at[b + 1 - 2 * core], hv.at[:, pl.ds(ND, ND)]),
                (gtab.at[a], gv),
            ]
        )
    ]
    loads[0].start()
    loads[1].start()
    scope("greet")
    barrier = pltpu.get_barrier_semaphore()
    for peer in PEERS:
        pl.semaphore_signal(barrier, inc=1, device_id=plane(peer)[0], device_id_type=MESH)
    far = (4, 3, 5, 2, 6, 1, 7)
    vars_ = {d: lax.rem(v + d, NVAR) for d in far}
    for d in far:
        pl.semaphore_signal(barrier, inc=1, device_id={"var": vars_[d]}, device_id_type=MESH)

    for load in loads[2:]:
        load.start()
    zacc[...] = jnp.zeros_like(zacc)
    scope("barrier")
    loads[0].wait()
    scope("barrier2")
    pl.semaphore_wait(barrier, PLANE - 1 + NVAR - 1)

    scope("send1")
    for i in range(PIECES):
        pltpu.make_async_remote_copy(
            src_ref=st.at[1, pl.ds(i * PIECE, PIECE)],
            dst_ref=xin.at[pl.ds(i * PIECE, PIECE)],
            send_sem=s1.at[0],
            recv_sem=r1.at[i],
            device_id={"lon": y * 2 + cores[1]},
            device_id_type=MESH,
        ).start()
    loads[5].wait()
    turned = jnp.transpose(bcol[...])
    for load in loads[1:5]:
        load.wait()

    for i in range(PIECES):
        scope(f"dft{i}")
        some = xin.at[pl.ds(i * PIECE, PIECE)]
        pltpu.make_async_copy(some, some, r1.at[i]).wait()
        chans = slice(i * PIECE, (i + 1) * PIECE)
        both = jnp.concatenate([st[0, chans], xin[chans]], axis=2).reshape(PIECE * RD, 2 * ND)
        lon = jnp.dot(both, ev[...], preferred_element_type=F32).astype(BF)
        for c in range(0, PIECE, 2):
            one, two = lon[c * RD : (c + 1) * RD], lon[(c + 1) * RD : (c + 2) * RD]
            pair = jnp.concatenate(
                [
                    jnp.concatenate([one[:, 0:128], two[:, 0:128]], axis=1),
                    jnp.concatenate([one[:, 128:256], two[:, 128:256]], axis=1),
                ],
                axis=0,
            )
            spec = jnp.dot(qv[...], pair, preferred_element_type=F32)
            at = (i * PIECE + c) * PITCH
            ss[at : at + PLANE * 6, :] = spec[:, 0:128]
            ss[at + PITCH : at + PITCH + PLANE * 6, :] = spec[:, 128:256]

    lane = lax.broadcasted_iota(jnp.int32, (CH, 128), 1)
    low, high = lane < 32, lane >= 96
    second = jnp.logical_and(lane >= 32, lane < 64)

    def pack(slot):
        t = [ss[pl.ds(slot * 6 + i, CH, stride=PITCH), :] for i in range(6)]
        up_r, half_r = pltpu.roll(t[2], 96, 1), pltpu.roll(t[2], 64, 1)
        up_i, half_i = pltpu.roll(t[5], 96, 1), pltpu.roll(t[5], 64, 1)
        p0, p1 = jnp.where(high, up_r, t[0]), jnp.where(high, half_r, t[1])
        p2, p3 = jnp.where(high, up_i, t[3]), jnp.where(high, half_i, t[4])
        p4 = jnp.where(low, half_r, jnp.where(second, up_i, 0.0))
        sa[slot] = jnp.concatenate([p0, p2], axis=1).astype(BF)
        sb[slot] = jnp.concatenate([p1, p3], axis=1).astype(BF)
        sc[slot] = (p4[0:8] + pltpu.roll(p4[8:16], 64, 1)).astype(BF)

    def copy2(src_ref, dst_ref, part, peer):
        to, slot = plane(peer)
        return pltpu.make_async_remote_copy(
            src_ref=src_ref.at[slot],
            dst_ref=dst_ref.at[me],
            send_sem=s2.at[part],
            recv_sem=r2.at[part],
            device_id=to,
            device_id_type=MESH,
        )

    scope("pack")
    for i in range(0, len(PEERS), 8):
        for peer in PEERS[i : i + 8]:
            pack(plane(peer)[1])
        for peer in PEERS[i : i + 8]:
            copy2(sa, ra, 0, peer).start()
    for peer in PEERS:
        copy2(sb, rb, 1, peer).start()
    for peer in PEERS:
        copy2(sc, rc, 2, peer).start()
    pack(me)
    ra[me] = sa[me]
    rb[me] = sb[me]
    rc[me] = sc[me]
    bias_r = jnp.broadcast_to(turned[:, 0:1], (256, 128))
    bias_i = jnp.broadcast_to(turned[:, 1:2], (256, 128))

    def whole_at(ref, sem):
        some = ref.at[pl.ds(0, PLANE - 1)]
        pltpu.make_async_copy(some, some, sem).wait()

    def others(ref, sem):
        some = ref.at[pl.ds(0, NVAR - 1)]
        return pltpu.make_async_copy(some, some, sem)

    for part, (got, every) in enumerate(((ra, xa), (rb, xb), (rc, xc))):
        scope(f"wait2_{part}")
        whole_at(got, r2.at[part])
        scope(f"sum_{part}")
        for half in range(2):
            total = got[half * CH].astype(F32)
            for i in range(1, CH):
                total += got[half * CH + i].astype(F32)
            rows = got.shape[1]
            every[v, half * rows : (half + 1) * rows] = total.astype(BF)
        for d in far:
            pltpu.make_async_remote_copy(
                src_ref=every.at[v],
                dst_ref=every.at[v],
                send_sem=s3.at[part],
                recv_sem=r3.at[part],
                device_id={"var": vars_[d]},
                device_id_type=MESH,
            ).start()

    scope("wait3")
    for load in loads[6:8]:
        load.wait()
    first = pl.multiple_of(v * CD, CD)
    own = jnp.concatenate([wov[0, pl.ds(first, CD), :], wov[1, pl.ds(first, CD), :]], axis=0)

    def combined(g, half):
        if g.shape[1] == 256:
            return g[:half, 0:128] - g[half:, 128:256], g[half:, 0:128] + g[:half, 128:256]
        which = lax.broadcasted_iota(jnp.int32, (half, 128), 1) < 32
        gr, gi = g[:half], g[half:]
        return (jnp.where(which, gr - pltpu.roll(gi, 96, 1), gr + pltpu.roll(gi, 32, 1)),)

    def mixed(every, part):
        others(every, r3.at[part]).wait()
        scope(f"mix_{part}")
        if every is xc:
            folded = xc[...].astype(F32).reshape(2 * NVAR, 8, 128)
            beside = pltpu.roll(folded, 64, 2)
            rows = jnp.stack([folded, beside], axis=1).reshape(256, 128).astype(BF)
        else:
            rows = every[...].reshape(256, -1)
        g = jnp.dot(wiv[...].reshape(512, 256), rows, preferred_element_type=F32)
        tiles = combined(g, 256)
        which = lax.broadcasted_iota(jnp.int32, (256, 128), 1) < 32
        biases = (bias_r, bias_i) if len(tiles) == 2 else (jnp.where(which, bias_r, bias_i),)
        hidden = jnp.concatenate([t + c for t, c in zip(tiles, biases)], axis=1)
        hidden = jnp.maximum(hidden, 0.0).astype(BF)
        return combined(jnp.dot(own, hidden, preferred_element_type=F32), CD)

    def copy4(src_ref, dst_ref, part, peer):
        to, slot = plane(peer)
        return pltpu.make_async_remote_copy(
            src_ref=src_ref.at[cores[peer[2]]],
            dst_ref=dst_ref.at[me],
            send_sem=s4.at[part],
            recv_sem=r4.at[part],
            device_id=to,
            device_id_type=MESH,
        )

    def spread(part, src_ref, dst_ref):
        scope(f"send4_{part}")
        for peer in PEERS:
            copy4(src_ref, dst_ref, part, peer).start()
        dst_ref[me] = src_ref[core]

    ma[...] = jnp.concatenate(mixed(xa, 0), axis=1).astype(BF).reshape(2, CH, 256)
    spread(0, ma, ba)
    scope("wait3_1")
    mb[...] = jnp.concatenate(mixed(xb, 1), axis=1).astype(BF).reshape(2, CH, 256)
    spread(1, mb, bb)
    scope("wait3_2")
    (last,) = mixed(xc, 2)
    last = jnp.where(lax.broadcasted_iota(jnp.int32, (CD, 128), 1) < 64, last, 0.0).reshape(2, 2, 8, 128)
    mc[...] = (last[:, 0] + pltpu.roll(last[:, 1], 64, 2)).astype(BF)
    spread(2, mc, bc)

    def put(owner, i, tile):
        ss[pl.ds(owner * 6 + i, CH, stride=PITCH), :] = tile

    for part, (got, i) in enumerate(((ba, 0), (bb, 1))):
        scope(f"wait4_{part}")
        whole_at(got, r4.at[part])
        scope(f"unpack_{part}")
        for o in range(PLANE):
            tiles = got[o].astype(F32)
            put(o, i, tiles[:, 0:128])
            put(o, i + 3, tiles[:, 128:256])
    scope("wait4_2")
    for load in loads[8:]:
        load.wait()
    whole_at(bc, r4.at[2])
    scope("unpack_2")
    mid = lane < 64
    for o in range(PLANE):
        one, two, folded = ba[o].astype(F32), bb[o].astype(F32), bc[o].astype(F32)
        end = jnp.concatenate([folded, pltpu.roll(folded, 64, 1)], axis=0)
        for i, cols, shift in ((2, slice(0, 128), 64), (5, slice(128, 256), 32)):
            start = jnp.where(low, pltpu.roll(one[:, cols], 32, 1), pltpu.roll(two[:, cols], 64, 1))
            put(o, i, jnp.where(mid, start, pltpu.roll(end, shift, 1)))

    column = lax.broadcasted_iota(jnp.int32, (RD, 128), 1)
    for c in range(0, CH, 2):
        if c % PIECE == 0:
            scope(f"gelu{c}")
        pair = jnp.concatenate(
            [ss[(c + i) * PITCH : (c + i) * PITCH + PLANE * 6, :] for i in range(2)], axis=1
        ).astype(BF)
        back = jnp.dot(rv[...], pair, preferred_element_type=F32).astype(BF)
        both = jnp.concatenate(
            [jnp.concatenate([back[0:RD, at], back[RD:, at]], axis=1) for at in (slice(0, 128), slice(128, 256))],
            axis=0,
        )
        act = gelu(jnp.dot(both, hv[...], preferred_element_type=F32))
        square = act * act
        for i in range(2):
            mine, at = act[i * RD : (i + 1) * RD], c + i
            field[0, core * CH + at] = mine[:, 0:128].astype(BF)
            fs[at] = mine[:, 128:256].astype(BF)
            total = jnp.sum(mine[:, 0:128] + mine[:, 128:256], axis=1, keepdims=True)
            zacc[0:RD, :] += jnp.where(column == at, total, 0.0)
            part = square[i * RD : (i + 1) * RD]
            part = (part[:, 0:128] + part[:, 128:256]) * gv[...]
            eacc[at] = jnp.sum(part.reshape(RD // 8, 8, 128), axis=0)
        if (c + 2) % PIECE == 0:
            first = c + 2 - PIECE
            pltpu.make_async_remote_copy(
                src_ref=fs.at[pl.ds(first, PIECE)],
                dst_ref=field.at[0, pl.ds(core * CH + first, PIECE)],
                send_sem=s5.at[0],
                recv_sem=r5.at[0],
                device_id={"lon": y * 2 + cores[1]},
                device_id_type=MESH,
            ).start()

    scope("stats")
    zmsg[...] = jnp.transpose(zacc[...])[0:CH]
    ones = jnp.ones((8, 128), F32)
    highest = dict(precision=lax.Precision.HIGHEST, preferred_element_type=F32)
    flat = lax.dot_general(ones, eacc[...].reshape(CH * 8, 128), (((1,), (1,)), ((), ())), **highest)
    channel = lax.div(lax.broadcasted_iota(jnp.int32, (128, 128), 0), 8) + core * CH
    pick = jnp.where(channel == lax.broadcasted_iota(jnp.int32, (128, 128), 1), 1.0, 0.0)
    emsg[...] = jnp.dot(flat, pick, **highest)[0:2]

    def copy6(peer):
        to, slot = plane(peer)
        return pltpu.make_async_remote_copy(
            src_ref=emsg,
            dst_ref=erec.at[me],
            send_sem=s6.at[0],
            recv_sem=r6.at[0],
            device_id=to,
            device_id_type=MESH,
        )

    def copy7(peer):
        to, _ = plane(peer)
        return pltpu.make_async_remote_copy(
            src_ref=zmsg,
            dst_ref=zrec.at[core * 4 + y],
            send_sem=s7.at[0],
            recv_sem=r7.at[0],
            device_id=to,
            device_id_type=MESH,
        )

    scope("send6")
    for peer in PEERS:
        copy6(peer).start()
    for peer in PEERS:
        if peer[0] == 0:
            copy7(peer).start()
    zrec[core * 4 + y] = zmsg[...]
    erec[me] = emsg[...]
    scope("wait5")
    pltpu.make_async_copy(xin, xin, s1.at[0]).wait()
    for part, (sent, every, spreads) in enumerate(((sa, xa, ba), (sb, xb, bb), (sc, xc, bc))):
        whole_at(sent, s2.at[part])
        others(every, s3.at[part]).wait()
        whole_at(spreads, s4.at[part])
    half = fs.at[pl.ds(0, CH)]
    pltpu.make_async_copy(half, half, s5.at[0]).wait()
    pltpu.make_async_copy(half, half, r5.at[0]).wait()
    scope("wait6")
    whole_at(erec, s6.at[0])
    seven = zrec.at[pl.ds(0, NLON - 1)]
    pltpu.make_async_copy(seven, seven, s7.at[0]).wait()
    pltpu.make_async_copy(seven, seven, r7.at[0]).wait()
    whole_at(erec, r6.at[0])
    scope(None)


def finish(total_area, field, rows, sums, out, zonal, energy, zv, evec, sems):
    big = pltpu.make_async_copy(field, out, sems.at[0])
    big.start()
    for half in range(2):
        total = rows[half * 4] + rows[half * 4 + 1] + rows[half * 4 + 2] + rows[half * 4 + 3]
        zv[0, half * CH : (half + 1) * CH, :] = total[:, 0:RD] * (1.0 / LON)
    small = pltpu.make_async_copy(zv, zonal, sems.at[1])
    small.start()
    gathered = sums[0]
    for i in range(1, PLANE):
        gathered += sums[i]
    evec[...] = gathered[0, 0:CD] * (1.0 / total_area)
    other = pltpu.make_async_copy(evec, energy, sems.at[2])
    other.start()
    big.wait()
    small.wait()
    other.wait()


def body(state, weights_in, bias_in, weights_out):
    *tabs, total_area = tables()
    hbm = pl.BlockSpec(memory_space=pltpu.HBM)
    vmem = pl.BlockSpec(memory_space=pltpu.VMEM)
    dma = pltpu.SemaphoreType.DMA
    operands = (state, *(jnp.asarray(t) for t in tabs), weights_in, bias_in, weights_out)
    field, rows, sums = pl.pallas_call(
        kernel,
        out_shape=(
            jax.ShapeDtypeStruct((1, CD, RD, ND), BF),
            jax.ShapeDtypeStruct((NLON, CH, 128), F32),
            jax.ShapeDtypeStruct((PLANE, 2, 128), F32),
        ),
        in_specs=[hbm] * 9,
        out_specs=(vmem, vmem, vmem),
        scratch_shapes=[
            pltpu.VMEM((2, CH, RD, ND), BF),
            pltpu.VMEM((2 * ND, 256), BF),
            pltpu.VMEM((PLANE * 6, 2 * RD), BF),
            pltpu.VMEM((2 * RD, PLANE * 6), BF),
            pltpu.VMEM((256, 2 * ND), BF),
            pltpu.VMEM((RD, 128), F32),
            pltpu.VMEM((2, 256, 256), BF),
            pltpu.VMEM((2, 256, 256), BF),
            pltpu.VMEM((128, 256), F32),
            pltpu.VMEM((CH, RD, ND), BF),
            pltpu.VMEM((CH * PITCH, 128), F32),
            pltpu.VMEM((PLANE, CH, 256), BF),
            pltpu.VMEM((PLANE, CH, 256), BF),
            pltpu.VMEM((PLANE, 8, 128), BF),
            pltpu.VMEM((PLANE, CH, 256), BF),
            pltpu.VMEM((PLANE, CH, 256), BF),
            pltpu.VMEM((PLANE, 8, 128), BF),
            pltpu.VMEM((NVAR, CD, 256), BF),
            pltpu.VMEM((NVAR, CD, 256), BF),
            pltpu.VMEM((NVAR, CH, 128), BF),
            pltpu.VMEM((2, CH, 256), BF),
            pltpu.VMEM((2, CH, 256), BF),
            pltpu.VMEM((2, 8, 128), BF),
            pltpu.VMEM((PLANE, CH, 256), BF),
            pltpu.VMEM((PLANE, CH, 256), BF),
            pltpu.VMEM((PLANE, 8, 128), BF),
            pltpu.VMEM((CH, RD, ND), BF),
            pltpu.VMEM((128, 128), F32),
            pltpu.VMEM((CH, 8, 128), F32),
            pltpu.VMEM((CH, 128), F32),
            pltpu.VMEM((2, 128), F32),
            dma((12,)),
        ]
        + [dma((1,)), dma((PIECES,)), dma((3,)), dma((3,)), dma((3,)), dma((3,))]
        + [dma((3,)), dma((3,))]
        + [dma((1,)), dma((1,))] * 3,
        compiler_params=pltpu.CompilerParams(
            collective_id=0, has_side_effects=True, vmem_limit_bytes=32 * 1024 * 1024
        ),
        name="spectral_layer",
    )(*(pltpu.with_memory_space_constraint(x, pltpu.HBM) for x in operands))
    return pl.pallas_call(
        lambda *refs: finish(total_area, *refs),
        out_shape=(
            jax.ShapeDtypeStruct((1, CD, RD, ND), BF),
            jax.ShapeDtypeStruct((1, CD, RD), F32),
            jax.ShapeDtypeStruct((CD,), F32),
        ),
        in_specs=[vmem, vmem, vmem],
        out_specs=(hbm, hbm, hbm),
        scratch_shapes=[
            pltpu.VMEM((1, CD, RD), F32),
            pltpu.VMEM((CD,), F32),
            dma((3,)),
        ],
        compiler_params=pltpu.CompilerParams(vmem_limit_bytes=8 * 1024 * 1024),
        name="finish",
    )(field, rows, sums)


def solution(mesh):
    return jax.shard_map(
        body,
        mesh=mesh,
        in_specs=(P(None, "var", "lat", "lon"), P(), P(), P()),
        out_specs=(P(None, "var", "lat", "lon"), P(None, "var", "lat"), P("var")),
        check_vma=False,
    )
```

```python
import math

import jax
import jax.numpy as jnp
import numpy as np
from jax import lax
from jax.experimental import pallas as pl
from jax.experimental.pallas import tpu as pltpu
from jax.sharding import PartitionSpec as P

LAT = 384
LON = 1024
MLAT = 96
MLON = 96
NVAR = 8
NLAT = 4
NLON = 8
PLANE = NLAT * NLON
CD = 32
RD = LAT // NLAT
ND = LON // NLON
JO = MLAT // PLANE
CH = CD // 2
PIECES = 2
PIECE = CH // PIECES
PITCH = PLANE * 6 + 8
MESH = pl.DeviceIdType.MESH
TAIL_AT = 0.23
TAIL = (
    0.09190782232377631,
    0.08914107185889676,
    0.10610870974692016,
    -0.0007481814870291388,
    0.25362340835459335,
    -0.23501017104744312,
    0.2688627946887361,
    -0.0738853870258165,
)
BF = jnp.bfloat16
F32 = jnp.float32


def ring(d):
    return min(d, 4 - d)


CHIPS = sorted(((i, j) for i in range(4) for j in range(4) if i or j), key=lambda c: -ring(c[0]) - ring(c[1]))
PEERS = [(i, j, c) for i, j in CHIPS for c in range(2)] + [(0, 0, 1)]


def gelu(x):
    size = jnp.abs(x)
    t = 1.0 / (1.0 + TAIL_AT * size)
    poly = TAIL[-1]
    for c in TAIL[-2::-1]:
        poly = poly * t + c
    tail = (size * t) * poly * jnp.exp2((x * x) * (-0.5 / math.log(2.0)))
    return jnp.maximum(x, 0.0) - tail


def tables():
    k = np.arange(MLON)
    n = np.arange(LON)
    angle = 2.0 * np.pi / LON * ((n[:, None] * k[None, :]) % LON)
    scale = 1.0 / math.sqrt(LAT * LON)
    etab = np.zeros((LON, 256), np.float32)
    etab[:, :MLON] = np.cos(angle) * scale
    etab[:, 128 : 128 + MLON] = -np.sin(angle) * scale
    weight = np.where(k == 0, 1.0, 2.0)[:, None] * scale
    full = np.zeros((256, LON), np.float32)
    full[:MLON] = weight * np.cos(angle.T)
    full[128 : 128 + MLON] = -weight * np.sin(angle.T)
    htab = full.reshape(256, NLON, ND).transpose(1, 0, 2)
    r = np.arange(LAT)
    freqs = np.arange(MLAT) - MLAT // 2
    turn = 2.0 * np.pi / LAT * np.mod(freqs[:, None] * r[None, :], LAT)
    cosine, sine = np.cos(turn), np.sin(turn)
    forward = np.zeros((PLANE, 6, 2, LAT), np.float32)
    forward[:, 0:3, 0] = cosine.reshape(PLANE, JO, LAT)
    forward[:, 0:3, 1] = sine.reshape(PLANE, JO, LAT)
    forward[:, 3:6, 0] = -sine.reshape(PLANE, JO, LAT)
    forward[:, 3:6, 1] = cosine.reshape(PLANE, JO, LAT)
    qtab = forward.reshape(PLANE * 6, 2, NLAT, RD).transpose(2, 0, 1, 3).reshape(NLAT, PLANE * 6, 2 * RD)
    rtab = qtab.transpose(0, 2, 1)
    area = np.cos(np.pi * ((r + 0.5) / LAT - 0.5))
    gtab = np.broadcast_to(area.reshape(NLAT, RD, 1), (NLAT, RD, 128))
    bf = lambda t: np.ascontiguousarray(t).astype(jnp.bfloat16)
    return (
        bf(etab),
        bf(qtab),
        bf(rtab),
        bf(htab),
        np.ascontiguousarray(gtab).astype(np.float32),
        float(LON * area.sum()),
    )


SCOPES = []


def scope(name):
    while SCOPES:
        SCOPES.pop().__exit__(None, None, None)
    if name:
        SCOPES.append(jax.named_scope(name))
        SCOPES[-1].__enter__()


def kernel(
    state,
    etab,
    qtab,
    rtab,
    htab,
    gtab,
    win,
    bias,
    wout,
    field,
    zrec,
    erec,
    st,
    ev,
    qv,
    rv,
    hv,
    gv,
    wiv,
    wov,
    bcol,
    xin,
    ss,
    sp,
    sc,
    rp,
    rc,
    xp,
    xc,
    ma,
    mb,
    mc,
    ba,
    bb,
    bc,
    fs,
    zacc,
    zmsg,
    emsg,
    load_sem,
    s1,
    r1,
    s2,
    r2,
    s3,
    r3,
    s4,
    r4,
    s5,
    r5,
    s6,
    r6,
    s7,
    r7,
):
    v = lax.axis_index("var")
    a = lax.axis_index("lat")
    b = lax.axis_index("lon")
    y, core = lax.div(b, 2), lax.rem(b, 2)

    def slot_of(pa, py, pc):
        return pc * 16 + pa * 4 + py

    me = slot_of(a, y, core)
    lats = [lax.rem(a + i, 4) for i in range(4)]
    ys = [lax.rem(y + i, 4) for i in range(4)]
    cores = [core, 1 - core]

    def plane(peer):
        i, j, c = peer
        pa, py, pc = lats[i], ys[j], cores[c]
        return {"lat": pa, "lon": py * 2 + pc}, slot_of(pa, py, pc)

    loads = [
        pltpu.make_async_copy(src, dst, load_sem.at[i])
        for i, (src, dst) in enumerate(
            [
                (state.at[0, pl.ds(CH * (1 - core), CH)], st.at[1]),
                (state.at[0, pl.ds(CH * core, CH)], st.at[0]),
                (etab.at[pl.ds(b * ND, ND)], ev.at[pl.ds(0, ND)]),
                (etab.at[pl.ds((b + 1 - 2 * core) * ND, ND)], ev.at[pl.ds(ND, ND)]),
                (qtab.at[a], qv),
                (bias, bcol.at[0:2]),
                (win, wiv),
                (wout, wov),
                (rtab.at[a], rv),
                (htab.at[b], hv.at[:, pl.ds(0, ND)]),
                (htab.at[b + 1 - 2 * core], hv.at[:, pl.ds(ND, ND)]),
                (gtab.at[a], gv),
            ]
        )
    ]
    loads[0].start()
    loads[1].start()
    scope("greet")
    barrier = pltpu.get_barrier_semaphore()
    for peer in PEERS:
        pl.semaphore_signal(barrier, inc=1, device_id=plane(peer)[0], device_id_type=MESH)
    far = (4, 3, 5, 2, 6, 1, 7)
    vars_ = {d: lax.rem(v + d, NVAR) for d in far}
    for d in far:
        pl.semaphore_signal(barrier, inc=1, device_id={"var": vars_[d]}, device_id_type=MESH)

    for load in loads[2:]:
        load.start()
    zacc[...] = jnp.zeros_like(zacc)
    scope("barrier")
    loads[0].wait()
    scope("barrier2")
    pl.semaphore_wait(barrier, PLANE - 1 + NVAR - 1)

    scope("send1")
    for i in range(PIECES):
        pltpu.make_async_remote_copy(
            src_ref=st.at[1, pl.ds(i * PIECE, PIECE)],
            dst_ref=xin.at[pl.ds(i * PIECE, PIECE)],
            send_sem=s1.at[0],
            recv_sem=r1.at[i],
            device_id={"lon": y * 2 + cores[1]},
            device_id_type=MESH,
        ).start()
    loads[5].wait()
    turned = jnp.transpose(bcol[...])
    for load in loads[1:5]:
        load.wait()

    for i in range(PIECES):
        scope(f"dft{i}")
        some = xin.at[pl.ds(i * PIECE, PIECE)]
        pltpu.make_async_copy(some, some, r1.at[i]).wait()
        chans = slice(i * PIECE, (i + 1) * PIECE)
        both = jnp.concatenate([st[0, chans], xin[chans]], axis=2).reshape(PIECE * RD, 2 * ND)
        lon = jnp.dot(both, ev[...], preferred_element_type=F32).astype(BF)
        for c in range(0, PIECE, 2):
            one, two = lon[c * RD : (c + 1) * RD], lon[(c + 1) * RD : (c + 2) * RD]
            pair = jnp.concatenate(
                [
                    jnp.concatenate([one[:, 0:128], two[:, 0:128]], axis=1),
                    jnp.concatenate([one[:, 128:256], two[:, 128:256]], axis=1),
                ],
                axis=0,
            )
            spec = jnp.dot(qv[...], pair, preferred_element_type=F32)
            at = (i * PIECE + c) * PITCH
            ss[at : at + PLANE * 6, :] = spec[:, 0:128]
            ss[at + PITCH : at + PITCH + PLANE * 6, :] = spec[:, 128:256]

    lane = lax.broadcasted_iota(jnp.int32, (CH, 128), 1)
    low, high = lane < 32, lane >= 96
    second = jnp.logical_and(lane >= 32, lane < 64)

    def pack(slot):
        t = [ss[pl.ds(slot * 6 + i, CH, stride=PITCH), :] for i in range(6)]
        up_r, half_r = pltpu.roll(t[2], 96, 1), pltpu.roll(t[2], 64, 1)
        up_i, half_i = pltpu.roll(t[5], 96, 1), pltpu.roll(t[5], 64, 1)
        p0, p1 = jnp.where(high, up_r, t[0]), jnp.where(high, half_r, t[1])
        p2, p3 = jnp.where(high, up_i, t[3]), jnp.where(high, half_i, t[4])
        p4 = jnp.where(low, half_r, jnp.where(second, up_i, 0.0))
        for i, p in enumerate((p0, p2, p1, p3)):
            sp[i, slot] = p.astype(BF)
        sc[slot] = (p4[0:8] + pltpu.roll(p4[8:16], 64, 1)).astype(BF)

    def copy2(src_ref, dst_ref, part, peer):
        to, slot = plane(peer)
        return pltpu.make_async_remote_copy(
            src_ref=src_ref.at[slot],
            dst_ref=dst_ref.at[me],
            send_sem=s2.at[part],
            recv_sem=r2.at[part],
            device_id=to,
            device_id_type=MESH,
        )

    scope("pack")
    done = 0
    for size in (3, 6, 8, 8, 6):
        for peer in PEERS[done : done + size]:
            pack(plane(peer)[1])
        for peer in PEERS[done : done + size]:
            copy2(sp.at[0], rp.at[0], 0, peer).start()
        done += size
    for i in range(1, 4):
        for peer in PEERS:
            copy2(sp.at[i], rp.at[i], i, peer).start()
    for peer in PEERS:
        copy2(sc, rc, 4, peer).start()
    pack(me)
    for i in range(4):
        rp[i, me] = sp[i, me]
    rc[me] = sc[me]
    bias_r = jnp.broadcast_to(turned[:, 0:1], (256, 128))
    bias_i = jnp.broadcast_to(turned[:, 1:2], (256, 128))

    def whole_at(ref, sem):
        some = ref.at[pl.ds(0, PLANE - 1)]
        pltpu.make_async_copy(some, some, sem).wait()

    def others(ref, sem):
        some = ref.at[pl.ds(0, NVAR - 1)]
        return pltpu.make_async_copy(some, some, sem)

    stages = [(sp.at[i], rp.at[i], xp.at[i]) for i in range(4)] + [(sc, rc, xc)]
    for part, (_, got, every) in enumerate(stages):
        scope(f"wait2_{part}")
        whole_at(got, r2.at[part])
        scope(f"sum_{part}")
        for half in range(2):
            total = got[half * CH].astype(F32)
            for i in range(1, CH):
                total += got[half * CH + i].astype(F32)
            rows = got.shape[1]
            every[v, half * rows : (half + 1) * rows] = total.astype(BF)
        for d in far:
            pltpu.make_async_remote_copy(
                src_ref=every.at[v],
                dst_ref=every.at[v],
                send_sem=s3.at[part],
                recv_sem=r3.at[part],
                device_id={"var": vars_[d]},
                device_id_type=MESH,
            ).start()

    scope("wait3")
    for load in loads[6:8]:
        load.wait()
    first = pl.multiple_of(v * CD, CD)
    own = jnp.concatenate([wov[0, pl.ds(first, CD), :], wov[1, pl.ds(first, CD), :]], axis=0)

    def combined(g, half):
        if g.shape[1] == 256:
            return g[:half, 0:128] - g[half:, 128:256], g[half:, 0:128] + g[:half, 128:256]
        which = lax.broadcasted_iota(jnp.int32, (half, 128), 1) < 32
        gr, gi = g[:half], g[half:]
        return (jnp.where(which, gr - pltpu.roll(gi, 96, 1), gr + pltpu.roll(gi, 32, 1)),)

    def mixed(*parts):
        for part in parts:
            others(stages[part][2], r3.at[part]).wait()
        scope(f"mix_{parts[0]}")
        if len(parts) == 1:
            folded = xc[...].astype(F32).reshape(2 * NVAR, 8, 128)
            beside = pltpu.roll(folded, 64, 2)
            rows = jnp.stack([folded, beside], axis=1).reshape(256, 128).astype(BF)
        else:
            rows = jnp.concatenate([xp[part].reshape(256, 128) for part in parts], axis=1)
        g = jnp.dot(wiv[...].reshape(512, 256), rows, preferred_element_type=F32)
        tiles = combined(g, 256)
        which = lax.broadcasted_iota(jnp.int32, (256, 128), 1) < 32
        biases = (bias_r, bias_i) if len(tiles) == 2 else (jnp.where(which, bias_r, bias_i),)
        hidden = jnp.concatenate([t + c for t, c in zip(tiles, biases)], axis=1)
        hidden = jnp.maximum(hidden, 0.0).astype(BF)
        return combined(jnp.dot(own, hidden, preferred_element_type=F32), CD)

    def copy4(src_ref, dst_ref, part, peer):
        to, slot = plane(peer)
        return pltpu.make_async_remote_copy(
            src_ref=src_ref.at[cores[peer[2]]],
            dst_ref=dst_ref.at[me],
            send_sem=s4.at[part],
            recv_sem=r4.at[part],
            device_id=to,
            device_id_type=MESH,
        )

    def spread(part, src_ref, dst_ref):
        scope(f"send4_{part}")
        for peer in PEERS:
            copy4(src_ref, dst_ref, part, peer).start()
        dst_ref[me] = src_ref[core]

    ma[...] = jnp.concatenate(mixed(0, 1), axis=1).astype(BF).reshape(2, CH, 256)
    spread(0, ma, ba)
    scope("wait3_1")
    mb[...] = jnp.concatenate(mixed(2, 3), axis=1).astype(BF).reshape(2, CH, 256)
    spread(1, mb, bb)
    scope("wait3_2")
    (last,) = mixed(4)
    last = jnp.where(lax.broadcasted_iota(jnp.int32, (CD, 128), 1) < 64, last, 0.0).reshape(2, 2, 8, 128)
    mc[...] = (last[:, 0] + pltpu.roll(last[:, 1], 64, 2)).astype(BF)
    spread(2, mc, bc)

    def put(owner, i, tile):
        ss[pl.ds(owner * 6 + i, CH, stride=PITCH), :] = tile

    def have(owner, i):
        return ss[pl.ds(owner * 6 + i, CH, stride=PITCH), :]

    scope("wait4_0")
    whole_at(ba, r4.at[0])
    scope("unpack_0")
    for o in range(PLANE):
        tiles = ba[o].astype(F32)
        for i, tile in ((0, tiles[:, 0:128]), (3, tiles[:, 128:256])):
            put(o, i, tile)
            put(o, i + 2, pltpu.roll(tile, 32, 1))
    scope("wait4_1")
    whole_at(bb, r4.at[1])
    scope("unpack_1")
    for o in range(PLANE):
        tiles = bb[o].astype(F32)
        for i, tile in ((1, tiles[:, 0:128]), (4, tiles[:, 128:256])):
            put(o, i, tile)
            put(o, i + 1, jnp.where(low, have(o, i + 1), pltpu.roll(tile, 64, 1)))
    scope("wait4_2")
    for load in loads[8:]:
        load.wait()
    whole_at(bc, r4.at[2])
    scope("unpack_2")
    mid = lane < 64
    for o in range(PLANE):
        folded = bc[o].astype(F32)
        turned_by = [pltpu.roll(folded, shift, 1) for shift in (64, 32, 96)]
        put(o, 2, jnp.where(mid, have(o, 2), jnp.concatenate([turned_by[0], folded], axis=0)))
        put(o, 5, jnp.where(mid, have(o, 5), jnp.concatenate(turned_by[1:], axis=0)))

    column = lax.broadcasted_iota(jnp.int32, (RD, 128), 1)
    powers = jnp.zeros((8, 128), F32)
    for c in range(0, CH, 2):
        if c % PIECE == 0:
            scope(f"gelu{c}")
        pair = jnp.concatenate(
            [ss[(c + i) * PITCH : (c + i) * PITCH + PLANE * 6, :] for i in range(2)], axis=1
        ).astype(BF)
        back = jnp.dot(rv[...], pair, preferred_element_type=F32).astype(BF)
        both = jnp.concatenate(
            [jnp.concatenate([back[0:RD, at], back[RD:, at]], axis=1) for at in (slice(0, 128), slice(128, 256))],
            axis=0,
        )
        act = gelu(jnp.dot(both, hv[...], preferred_element_type=F32))
        square = act * act
        for i in range(2):
            mine, at = act[i * RD : (i + 1) * RD], c + i
            field[0, core * CH + at] = mine[:, 0:128].astype(BF)
            fs[at] = mine[:, 128:256].astype(BF)
            total = jnp.sum(mine[:, 0:128] + mine[:, 128:256], axis=1, keepdims=True)
            zacc[0:RD, :] += jnp.where(column == at, total, 0.0)
            part = square[i * RD : (i + 1) * RD]
            part = (part[:, 0:128] + part[:, 128:256]) * gv[...]
            part = jnp.sum(jnp.sum(part.reshape(RD // 8, 8, 128), axis=0), axis=1, keepdims=True)
            powers += jnp.where(column[0:8] == core * CH + at, part, 0.0)
        if (c + 2) % PIECE == 0:
            first = c + 2 - PIECE
            pltpu.make_async_remote_copy(
                src_ref=fs.at[pl.ds(first, PIECE)],
                dst_ref=field.at[0, pl.ds(core * CH + first, PIECE)],
                send_sem=s5.at[0],
                recv_sem=r5.at[0],
                device_id={"lon": y * 2 + cores[1]},
                device_id_type=MESH,
            ).start()

    scope("stats")
    zmsg[...] = jnp.transpose(zacc[...])[0:CH]
    emsg[...] = jnp.broadcast_to(jnp.sum(powers, axis=0, keepdims=True), (2, 128))

    def copy6(peer):
        to, slot = plane(peer)
        return pltpu.make_async_remote_copy(
            src_ref=emsg,
            dst_ref=erec.at[me],
            send_sem=s6.at[0],
            recv_sem=r6.at[0],
            device_id=to,
            device_id_type=MESH,
        )

    def copy7(peer):
        to, _ = plane(peer)
        return pltpu.make_async_remote_copy(
            src_ref=zmsg,
            dst_ref=zrec.at[core * 4 + y],
            send_sem=s7.at[0],
            recv_sem=r7.at[0],
            device_id=to,
            device_id_type=MESH,
        )

    scope("send6")
    for peer in PEERS:
        copy6(peer).start()
    for peer in PEERS:
        if peer[0] == 0:
            copy7(peer).start()
    zrec[core * 4 + y] = zmsg[...]
    erec[me] = emsg[...]
    scope("wait5")
    pltpu.make_async_copy(xin, xin, s1.at[0]).wait()
    for part, (sent, _, every) in enumerate(stages):
        whole_at(sent, s2.at[part])
        others(every, s3.at[part]).wait()
    for part, spreads in enumerate((ba, bb, bc)):
        whole_at(spreads, s4.at[part])
    half = fs.at[pl.ds(0, CH)]
    pltpu.make_async_copy(half, half, s5.at[0]).wait()
    pltpu.make_async_copy(half, half, r5.at[0]).wait()
    scope("wait6")
    whole_at(erec, s6.at[0])
    seven = zrec.at[pl.ds(0, NLON - 1)]
    pltpu.make_async_copy(seven, seven, s7.at[0]).wait()
    pltpu.make_async_copy(seven, seven, r7.at[0]).wait()
    whole_at(erec, r6.at[0])
    scope(None)


def finish(total_area, field, rows, sums, out, zonal, energy, zv, evec, sems):
    big = pltpu.make_async_copy(field, out, sems.at[0])
    big.start()
    for half in range(2):
        total = rows[half * 4] + rows[half * 4 + 1] + rows[half * 4 + 2] + rows[half * 4 + 3]
        zv[0, half * CH : (half + 1) * CH, :] = total[:, 0:RD] * (1.0 / LON)
    small = pltpu.make_async_copy(zv, zonal, sems.at[1])
    small.start()
    gathered = sums[0]
    for i in range(1, PLANE):
        gathered += sums[i]
    evec[...] = gathered[0, 0:CD] * (1.0 / total_area)
    other = pltpu.make_async_copy(evec, energy, sems.at[2])
    other.start()
    big.wait()
    small.wait()
    other.wait()


def body(state, weights_in, bias_in, weights_out):
    *tabs, total_area = tables()
    hbm = pl.BlockSpec(memory_space=pltpu.HBM)
    vmem = pl.BlockSpec(memory_space=pltpu.VMEM)
    dma = pltpu.SemaphoreType.DMA
    operands = (state, *(jnp.asarray(t) for t in tabs), weights_in, bias_in, weights_out)
    field, rows, sums = pl.pallas_call(
        kernel,
        out_shape=(
            jax.ShapeDtypeStruct((1, CD, RD, ND), BF),
            jax.ShapeDtypeStruct((NLON, CH, 128), F32),
            jax.ShapeDtypeStruct((PLANE, 2, 128), F32),
        ),
        in_specs=[hbm] * 9,
        out_specs=(vmem, vmem, vmem),
        scratch_shapes=[
            pltpu.VMEM((2, CH, RD, ND), BF),
            pltpu.VMEM((2 * ND, 256), BF),
            pltpu.VMEM((PLANE * 6, 2 * RD), BF),
            pltpu.VMEM((2 * RD, PLANE * 6), BF),
            pltpu.VMEM((256, 2 * ND), BF),
            pltpu.VMEM((RD, 128), F32),
            pltpu.VMEM((2, 256, 256), BF),
            pltpu.VMEM((2, 256, 256), BF),
            pltpu.VMEM((128, 256), F32),
            pltpu.VMEM((CH, RD, ND), BF),
            pltpu.VMEM((CH * PITCH, 128), F32),
            pltpu.VMEM((4, PLANE, CH, 128), BF),
            pltpu.VMEM((PLANE, 8, 128), BF),
            pltpu.VMEM((4, PLANE, CH, 128), BF),
            pltpu.VMEM((PLANE, 8, 128), BF),
            pltpu.VMEM((4, NVAR, CD, 128), BF),
            pltpu.VMEM((NVAR, CH, 128), BF),
            pltpu.VMEM((2, CH, 256), BF),
            pltpu.VMEM((2, CH, 256), BF),
            pltpu.VMEM((2, 8, 128), BF),
            pltpu.VMEM((PLANE, CH, 256), BF),
            pltpu.VMEM((PLANE, CH, 256), BF),
            pltpu.VMEM((PLANE, 8, 128), BF),
            pltpu.VMEM((CH, RD, ND), BF),
            pltpu.VMEM((128, 128), F32),
            pltpu.VMEM((CH, 128), F32),
            pltpu.VMEM((2, 128), F32),
            dma((12,)),
        ]
        + [dma((1,)), dma((PIECES,)), dma((5,)), dma((5,)), dma((5,)), dma((5,))]
        + [dma((3,)), dma((3,))]
        + [dma((1,)), dma((1,))] * 3,
        compiler_params=pltpu.CompilerParams(
            collective_id=0, has_side_effects=True, vmem_limit_bytes=32 * 1024 * 1024
        ),
        name="spectral_layer",
    )(*(pltpu.with_memory_space_constraint(x, pltpu.HBM) for x in operands))
    return pl.pallas_call(
        lambda *refs: finish(total_area, *refs),
        out_shape=(
            jax.ShapeDtypeStruct((1, CD, RD, ND), BF),
            jax.ShapeDtypeStruct((1, CD, RD), F32),
            jax.ShapeDtypeStruct((CD,), F32),
        ),
        in_specs=[vmem, vmem, vmem],
        out_specs=(hbm, hbm, hbm),
        scratch_shapes=[
            pltpu.VMEM((1, CD, RD), F32),
            pltpu.VMEM((CD,), F32),
            dma((3,)),
        ],
        compiler_params=pltpu.CompilerParams(vmem_limit_bytes=8 * 1024 * 1024),
        name="finish",
    )(field, rows, sums)


def solution(mesh):
    return jax.shard_map(
        body,
        mesh=mesh,
        in_specs=(P(None, "var", "lat", "lon"), P(), P(), P()),
        out_specs=(P(None, "var", "lat", "lon"), P(None, "var", "lat"), P("var")),
        check_vma=False,
    )
```
